32 devices in a mesh: slab: 8 (over z, y), sub: 4 (over x, core).
Axes of the slice: x: 2, y: 2, z: 4, core: 2. Of those that a mesh axis runs over, the one named last changes fastest.
Arguments:
- factor_obs: float32 [32, 64, 64, 512], P('slab', 'sub'), may hold values from -0.20992233 to 0.20992233
- factor_ctrl: float32 [32, 64, 64, 512], P('slab', 'sub'), may hold values from -0.20992233 to 0.20992233
- diffusivity: float32 [32, 4096], P('slab', 'sub'), may hold values from 0.5 to 2
- input_map: float32 [4, 32, 4096], P(None, 'slab', 'sub'), may hold values from -2 to 2
- output_map: float32 [4, 32, 4096], P(None, 'slab', 'sub'), may hold values from -2 to 2
- start_block: float32 [512, 128], replicated, may hold values from -6 to 6
- order: int32 [1], replicated, may hold values from 64 to 128
Outputs:
- reduced_mass: float32 [128, 128], replicated
- reduced_state: float32 [128, 128], replicated
- reduced_input: float32 [128, 4], replicated
- reduced_output: float32 [4, 128], replicated
The draws below stay inside these ranges and needn't reach their ends.
All inputs are finite; a program needn't handle non-finite values.
Results may differ from the reference program's by a relative error of at most 0.00017.
Values sent between devices are 32-bit elements; how exact they have to be, the bound alone decides.
A program may use at most 128 MiB of HBM per device.

```python
import math
import jax
import jax.numpy as jnp
from jax import lax

NX = 64
RANK = 512
RMAX = 128
NIN = 4
NOUT = 4
POWER = 2
NZ = 32
NY = 64
NYX = 4096
NCELL = 131072


def factor_draw(key, salt):
    key = jax.random.fold_in(key, salt)
    entry_key, level_key = jax.random.split(key)
    entries = jnp.clip(jax.random.normal(entry_key, (NZ, NY, NX, RANK), jnp.float32), -6.0, 6.0)
    level = jax.random.uniform(level_key, (NZ, NY, NX), jnp.float32) * math.log(10.0)
    rising = 1.0 + 2.0 * jnp.arange(NZ, dtype=jnp.float32) / max(NZ - 1, 1)
    scales = jnp.exp(level) * rising[:, None, None] / 9.65 * float(NCELL * RANK) ** (-0.25)
    return (entries * scales[..., None]).astype(jnp.float32)


def draw_factor_obs(key, part):
    return factor_draw(key, 11)


def draw_factor_ctrl(key, part):
    return factor_draw(key, 23)


def block_levels(rng, dims, pieces, smallest, high):
    def one(dim, parts):
        heights = jax.random.uniform(jax.random.fold_in(jax.random.fold_in(rng, 6), dim), (parts,), jnp.float32, smallest / len(pieces), high / len(pieces))
        return jnp.repeat(jnp.exp(heights), dims[dim] // parts).reshape((-1,) + (1,) * (len(dims) - dim - 1))

    level = one(*pieces[0])
    for cut in pieces[1:]:
        level = level * one(*cut)
    return level


def centred(rng, shape, spread, limit, cuts=(), kind=jnp.bfloat16):
    values = spread * jax.random.normal(rng, shape, jnp.float32)
    if cuts:
        values = values * block_levels(rng, shape, cuts, -0.22, 0.18)
    return jnp.clip(values, -limit, limit).astype(kind)


def setup_inputs(seed: int = 0) -> dict:
    key_list = jax.random.split(jax.random.key(seed), 8)
    factor_obs = draw_factor_obs(jax.random.fold_in(key_list[7], 71), 0)
    factor_ctrl = draw_factor_ctrl(jax.random.fold_in(key_list[7], 71), 0)
    diffusivity = jnp.clip(jnp.exp(math.log(2.0) - 1.3862944 * jax.random.uniform(key_list[2], (NZ, NYX), jnp.float32) ** block_levels(key_list[2], (NZ, NYX), ((0, 8), (1, 4)), -0.2, 0.2)), 0.5, 2.0)
    input_map = centred(key_list[3], (NIN, NZ, NYX), (max(NCELL // RANK // 32, 1)) ** -0.5, 2.0, ((1, 8), (2, 4)), jnp.float32)
    output_map = centred(key_list[4], (NOUT, NZ, NYX), (max(NCELL // RANK // 32, 1)) ** -0.5, 2.0, ((1, 8), (2, 4)), jnp.float32)
    start_block = centred(key_list[5], (RANK, RMAX), 1.0, 6.0, (), jnp.float32)
    order = jax.random.randint(key_list[6], (1,), RMAX // 2, RMAX + 1).astype(jnp.int32)
    return dict(factor_obs=factor_obs, factor_ctrl=factor_ctrl, diffusivity=diffusivity, input_map=input_map, output_map=output_map, start_block=start_block, order=order)


def matmul(first, second):
    return jnp.dot(first.astype(jnp.float32), second.astype(jnp.float32), precision=lax.Precision.HIGHEST, preferred_element_type=jnp.float32)

def orthonormal(start):
    gram = matmul(start.T, start)
    lower_factor = jnp.linalg.cholesky(gram)
    return lax.linalg.triangular_solve(lower_factor, start, left_side=False, lower=True, transpose_a=True)

def subspace_bases(cross_gram, start_block):
    right_basis = orthonormal(matmul(cross_gram.T, start_block))
    left_basis = orthonormal(matmul(cross_gram, right_basis))
    for repeat in range(POWER - 1):
        right_basis = orthonormal(matmul(cross_gram.T, left_basis))
        left_basis = orthonormal(matmul(cross_gram, right_basis))
    return (left_basis, right_basis)

def apply_stencil(field, conduct):
    padded = jnp.pad(field, ((1, 1), (1, 1), (1, 1), (0, 0)))
    center = padded[1:-1, 1:-1, 1:-1]
    beside = padded[2:, 1:-1, 1:-1] + padded[:-2, 1:-1, 1:-1]
    beside = beside + padded[1:-1, 2:, 1:-1] + padded[1:-1, :-2, 1:-1]
    beside = beside + padded[1:-1, 1:-1, 2:] + padded[1:-1, 1:-1, :-2]
    return conduct[..., None] * (beside - 6.0 * center) / 6.0

def reference(factor_obs, factor_ctrl, diffusivity, input_map, output_map, start_block, order):
    cell_count = NZ * NY * NX
    observe = factor_obs.reshape(cell_count, RANK)
    control = factor_ctrl.reshape(cell_count, RANK)
    cross_gram = matmul(observe.T, control)
    left_basis, right_basis = subspace_bases(cross_gram, start_block)
    ctrl_space = matmul(control, right_basis)
    obs_space = matmul(observe, left_basis)
    conduct = diffusivity.reshape(NZ, NY, NX)
    applied = apply_stencil(ctrl_space.reshape(NZ, NY, NX, RMAX), conduct).reshape(cell_count, RMAX)
    kept_mask = (jnp.arange(RMAX, dtype=jnp.int32) < order[0]).astype(jnp.float32)
    square_mask = kept_mask[:, None] * kept_mask[None, :]
    reduced_mass = square_mask * matmul(left_basis.T, matmul(cross_gram, right_basis))
    reduced_state = square_mask * matmul(obs_space.T, applied)
    drive = input_map.reshape(NIN, cell_count)
    sense = output_map.reshape(NOUT, cell_count)
    reduced_input = kept_mask[:, None] * matmul(drive, obs_space).T
    reduced_output = kept_mask[None, :] * matmul(sense, ctrl_space)
    return (reduced_mass, reduced_state, reduced_input, reduced_output)
```

```python
import functools
import jax
import jax.numpy as jnp
from jax import lax
from jax.experimental import pallas as pl
from jax.experimental.pallas import tpu as pltpu
from jax.sharding import PartitionSpec as P

LANES = 128
SUBS = 8
PANEL = 16
HIGHEST = lax.Precision.HIGHEST
HIGH = lax.Precision.HIGH


def exact(first, second, dims=((1,), (0,))):
    return lax.dot_general(
        first, second, (dims, ((), ())), precision=HIGHEST, preferred_element_type=jnp.float32
    )


def tall(first, second, dims=((1,), (0,))):
    return lax.dot_general(
        first, second, (dims, ((), ())), precision=HIGH, preferred_element_type=jnp.float32
    )


def narrow(first, second, dims=((1,), (0,))):
    return lax.dot_general(first, second, (dims, ((), ())), preferred_element_type=jnp.float32)


def three_parts(value):
    high = value.astype(jnp.bfloat16).astype(jnp.float32)
    mid = (value - high).astype(jnp.bfloat16).astype(jnp.float32)
    return high, mid, value - high - mid


def two_parts(value):
    high = value.astype(jnp.bfloat16)
    return high, (value - high.astype(jnp.float32)).astype(jnp.bfloat16)


def three_dots(first, second, dims=((1,), (0,))):
    (a, b), (c, d) = two_parts(first), two_parts(second)
    return narrow(a, c, dims) + (narrow(a, d, dims) + narrow(b, c, dims))


def gram_kernel(first_ref, second_ref, out_ref):
    @pl.when(pl.program_id(0) == 0)
    def _():
        out_ref[...] = jnp.zeros_like(out_ref)

    out_ref[...] += three_dots(first_ref[...], second_ref[...], ((0,), (0,)))


def cells_step(cells):
    return 512 if cells % 512 == 0 else cells


def gram(first, second):
    cells, wide = first.shape
    step = cells_step(cells)
    spec = pl.BlockSpec((step, wide), lambda k: (k, 0))
    return pl.pallas_call(
        gram_kernel,
        grid=(cells // step,),
        out_shape=jax.ShapeDtypeStruct((wide, second.shape[1]), jnp.float32),
        in_specs=[spec, spec],
        out_specs=pl.BlockSpec((wide, second.shape[1]), lambda k: (0, 0)),
        compiler_params=pltpu.CompilerParams(dimension_semantics=("arbitrary",)),
    )(first, second)


def sub_bits(count):
    return [1 << b for b in range(count.bit_length() - 1)]


def all_reduce_kernel(nslab, nsub, in_ref, out_ref, work, got_sub, got_slab, *sems):
    rs_sub_send, rs_sub_recv, rs_slab_send, rs_slab_recv = sems[:4]
    ag_slab_send, ag_slab_recv, ag_sub_send, ag_sub_recv = sems[4:]
    slab, sub = lax.axis_index("slab"), lax.axis_index("sub")
    rows, cols = work.shape[0], in_ref.shape[1]
    bits = sub_bits(nsub)

    def partner(bit):
        has = lax.rem(sub // bit, 2)
        return has, sub + bit - 2 * bit * has

    barrier = pltpu.get_barrier_semaphore()
    for bit in bits:
        pl.semaphore_signal(barrier, inc=1, device_id={"sub": partner(bit)[1]})
    for off in range(1, nslab):
        pl.semaphore_signal(barrier, inc=1, device_id={"slab": lax.rem(slab + off, nslab)})

    tall_rows = in_ref.shape[0]
    for c in range(cols // LANES):
        work[c * tall_rows : (c + 1) * tall_rows, :] = in_ref[:, c * LANES : (c + 1) * LANES]
    pl.semaphore_wait(barrier, len(bits) + nslab - 1)

    base, length, taken = 0, rows, 0
    for s, bit in enumerate(bits):
        half = length // 2
        has, other = partner(bit)
        keep = pl.multiple_of(base + has * half, 8)
        give = pl.multiple_of(base + (1 - has) * half, 8)
        copy = pltpu.make_async_remote_copy(
            src_ref=work.at[pl.ds(give, half)],
            dst_ref=got_sub.at[pl.ds(taken, half)],
            send_sem=rs_sub_send.at[s],
            recv_sem=rs_sub_recv.at[s],
            device_id={"sub": other},
        )
        copy.start()
        copy.wait()
        work[pl.ds(keep, half), :] += got_sub[taken : taken + half, :]
        base, length, taken = keep, half, taken + half

    piece = length // nslab
    copies = []
    for off in range(1, nslab):
        peer = lax.rem(slab + off, nslab)
        copy = pltpu.make_async_remote_copy(
            src_ref=work.at[pl.ds(pl.multiple_of(base + peer * piece, 8), piece)],
            dst_ref=got_slab.at[off],
            send_sem=rs_slab_send.at[off],
            recv_sem=rs_slab_recv.at[off],
            device_id={"slab": peer},
        )
        copy.start()
        copies.append(copy)
    mine = pl.multiple_of(base + slab * piece, 8)
    total = work[pl.ds(mine, piece), :]
    for off in range(1, nslab):
        copies[off - 1].wait_recv()
        total = total + got_slab[off]
    out_ref[pl.ds(mine, piece), :] = total
    for copy in copies:
        copy.wait_send()

    copies = []
    for off in range(1, nslab):
        copy = pltpu.make_async_remote_copy(
            src_ref=out_ref.at[pl.ds(mine, piece)],
            dst_ref=out_ref.at[pl.ds(mine, piece)],
            send_sem=ag_slab_send.at[off],
            recv_sem=ag_slab_recv.at[off],
            device_id={"slab": lax.rem(slab + off, nslab)},
        )
        copy.start()
        copies.append(copy)
    for copy in copies:
        copy.wait()

    for s in reversed(range(len(bits))):
        has, other = partner(bits[s])
        copy = pltpu.make_async_remote_copy(
            src_ref=out_ref.at[pl.ds(base, length)],
            dst_ref=out_ref.at[pl.ds(base, length)],
            send_sem=ag_sub_send.at[s],
            recv_sem=ag_sub_recv.at[s],
            device_id={"sub": other},
        )
        copy.start()
        copy.wait()
        base = pl.multiple_of(base - has * length, 8)
        length = 2 * length


def all_reduce(part, ident):
    nslab, nsub = lax.axis_size("slab"), lax.axis_size("sub")
    rows = part.shape[0] * (part.shape[1] // LANES)
    bits = len(sub_bits(nsub))
    piece = rows // (nsub * nslab)
    sub_sem, slab_sem = pltpu.SemaphoreType.DMA((bits,)), pltpu.SemaphoreType.DMA((nslab,))
    return pl.pallas_call(
        functools.partial(all_reduce_kernel, nslab, nsub),
        out_shape=jax.ShapeDtypeStruct((rows, LANES), jnp.float32),
        in_specs=[pl.BlockSpec(memory_space=pltpu.VMEM)],
        out_specs=pl.BlockSpec(memory_space=pltpu.VMEM),
        scratch_shapes=[
            pltpu.VMEM((rows, LANES), jnp.float32),
            pltpu.VMEM((rows, LANES), jnp.float32),
            pltpu.VMEM((nslab, piece, LANES), jnp.float32),
            sub_sem, sub_sem, slab_sem, slab_sem, slab_sem, slab_sem, sub_sem, sub_sem,
        ],
        compiler_params=pltpu.CompilerParams(collective_id=ident, has_side_effects=True),
    )(part)


def small_kernel(nslab, nsub, in_ref, out_ref, total, slots, got_slab, *sems):
    sub_send, sub_recv, rs_send, rs_recv, ag_send, ag_recv = sems
    slab, sub = lax.axis_index("slab"), lax.axis_index("sub")
    barrier = pltpu.get_barrier_semaphore()
    for off in range(1, nsub):
        pl.semaphore_signal(barrier, inc=1, device_id={"sub": lax.rem(sub + off, nsub)})
    for off in range(1, nslab):
        pl.semaphore_signal(barrier, inc=1, device_id={"slab": lax.rem(slab + off, nslab)})
    pl.semaphore_wait(barrier, nsub + nslab - 2)

    copies = []
    for off in range(1, nsub):
        copy = pltpu.make_async_remote_copy(
            src_ref=in_ref,
            dst_ref=slots.at[sub],
            send_sem=sub_send.at[off],
            recv_sem=sub_recv.at[off],
            device_id={"sub": lax.rem(sub + off, nsub)},
        )
        copy.start()
        copies.append(copy)
    slots[sub] = in_ref[...]
    for copy in copies:
        copy.wait()
    value = slots[0]
    for k in range(1, nsub):
        value = value + slots[k]
    total[...] = value

    piece = in_ref.shape[0] // nslab
    copies = []
    for off in range(1, nslab):
        peer = lax.rem(slab + off, nslab)
        copy = pltpu.make_async_remote_copy(
            src_ref=total.at[pl.ds(pl.multiple_of(peer * piece, 8), piece)],
            dst_ref=got_slab.at[off],
            send_sem=rs_send.at[off],
            recv_sem=rs_recv.at[off],
            device_id={"slab": peer},
        )
        copy.start()
        copies.append(copy)
    mine = pl.multiple_of(slab * piece, 8)
    value = total[pl.ds(mine, piece), :]
    for off in range(1, nslab):
        copies[off - 1].wait()
        value = value + got_slab[off]
    out_ref[pl.ds(mine, piece), :] = value
    copies = []
    for off in range(1, nslab):
        copy = pltpu.make_async_remote_copy(
            src_ref=out_ref.at[pl.ds(mine, piece)],
            dst_ref=out_ref.at[pl.ds(mine, piece)],
            send_sem=ag_send.at[off],
            recv_sem=ag_recv.at[off],
            device_id={"slab": lax.rem(slab + off, nslab)},
        )
        copy.start()
        copies.append(copy)
    for copy in copies:
        copy.wait()


def small_all_reduce(part, ident):
    nslab, nsub = lax.axis_size("slab"), lax.axis_size("sub")
    rows = part.shape[0]
    sub_sem, slab_sem = pltpu.SemaphoreType.DMA((nsub,)), pltpu.SemaphoreType.DMA((nslab,))
    return pl.pallas_call(
        functools.partial(small_kernel, nslab, nsub),
        out_shape=jax.ShapeDtypeStruct((rows, LANES), jnp.float32),
        in_specs=[pl.BlockSpec(memory_space=pltpu.VMEM)],
        out_specs=pl.BlockSpec(memory_space=pltpu.VMEM),
        scratch_shapes=[
            pltpu.VMEM((rows, LANES), jnp.float32),
            pltpu.VMEM((nsub, rows, LANES), jnp.float32),
            pltpu.VMEM((nslab, rows // nslab, LANES), jnp.float32),
            sub_sem, sub_sem, slab_sem, slab_sem, slab_sem, slab_sem,
        ],
        compiler_params=pltpu.CompilerParams(collective_id=ident, has_side_effects=True),
    )(part)


def across(block, sub):
    return jnp.broadcast_to(block[sub : sub + 1, :], block.shape)

def column(rows, lane):
    return jnp.broadcast_to(rows[:, lane : lane + 1], (SUBS, LANES))

def inverse_factor(work, size):
    wide = 2 * size // LANES
    place = lax.broadcasted_iota(jnp.int32, (SUBS, 2 * size), 0)
    spread = lambda x: jnp.concatenate([x] * wide, axis=1)
    carried = [work[h * SUBS : (h + 1) * SUBS, :] for h in range(2)]
    for base in range(0, size, PANEL):
        low, high = carried
        cols_low = [column(low, base + j) for j in range(SUBS)]
        cols_high = [column(high, base + j) for j in range(PANEL)]
        panel_low, panel_high = low, high
        scales, rows, leads = [], [], []
        for j in range(PANEL):
            if j < SUBS:
                scale = lax.rsqrt(across(cols_low[j], j))
                lead_low = cols_low[j] * scale
                row = across(low, j) * spread(scale)
                panel_low = jnp.where(place == j, row, panel_low)
            else:
                scale = lax.rsqrt(across(cols_high[j], j - SUBS))
                row = across(high, j - SUBS) * spread(scale)
                panel_high = jnp.where(place == j - SUBS, row, panel_high)
            lead_high = cols_high[j] * scale
            lead = {}
            for m in range(j + 1, PANEL):
                if m < SUBS:
                    lead[m] = across(lead_low, m)
                    cols_low[m] = cols_low[m] - lead_low * lead[m]
                else:
                    lead[m] = across(lead_high, m - SUBS)
                cols_high[m] = cols_high[m] - lead_high * lead[m]
            if j < SUBS - 1:
                low = low - spread(lead_low) * row
            if j < PANEL - 1:
                high = high - spread(lead_high) * row
            scales.append(scale)
            rows.append(row)
            leads.append(lead)
        panel = jnp.concatenate([panel_low, panel_high], axis=0)
        work[base : base + PANEL, :] = panel
        if base + PANEL < size:
            start = base + PANEL
            carried = []
            for h in range(2):
                rest = work[start + h * SUBS : start + (h + 1) * SUBS, :]
                cols = [column(rest, base + j) for j in range(PANEL)]
                for j in range(PANEL):
                    lead_rest = cols[j] * scales[j]
                    for m in range(j + 1, PANEL):
                        cols[m] = cols[m] - lead_rest * leads[j][m]
                    rest = rest - spread(lead_rest) * rows[j]
                carried.append(rest)
        if base + 2 * PANEL < size:
            start = base + 2 * PANEL
            high, mid, low = three_parts(panel)
            first = jnp.concatenate([high, high, mid, high, low, mid], axis=0)[:, :size]
            second = jnp.concatenate([high, mid, high, low, high, mid], axis=0)
            update = narrow(first.astype(jnp.bfloat16), second.astype(jnp.bfloat16), ((0,), (0,)))
            work[start:, :] = work[start:, :] - update[start:, :]


def pair(value):
    return jnp.concatenate(two_parts(value), axis=1)


def fold(wide, size):
    return wide[:, :size] + wide[:, size:]


def apply_parts(high, low, block):
    size = block.shape[1]
    parts = pair(block)
    return fold(narrow(high, parts) + narrow(low, parts), size)


def gram_parts(parts):
    size = parts.shape[1] // 2
    full = narrow(parts, parts, ((0,), (0,)))
    return (full[:size, :size] + full[size:, size:]) + (full[:size, size:] + full[size:, :size])


def right_apply(parts, factor):
    turned = pair(factor.T)
    return fold(narrow(parts, jnp.concatenate([turned, turned], axis=0)), factor.shape[0])


def bases_kernel(sweeps, gram_ref, start_ref, left_ref, right_ref, mass_ref, both_high, both_low, block, work):
    rank, size = start_ref.shape
    for c in range(rank // LANES):
        cols = slice(c * LANES, (c + 1) * LANES)
        tile = gram_ref[c * rank : (c + 1) * rank, :]
        high, low = two_parts(tile)
        both_high[1, :, cols] = high
        both_low[1, :, cols] = low
        high, low = two_parts(tile.T)
        both_high[0, cols, :] = high
        both_low[0, cols, :] = low
    block[...] = start_ref[...]
    row = lax.broadcasted_iota(jnp.int32, (size, size), 0)
    col = lax.broadcasted_iota(jnp.int32, (size, size), 1)
    eye = (row == col).astype(jnp.float32)

    def step(k, carry):
        turn = lax.rem(k, 2)
        parts = pair(apply_parts(both_high[turn], both_low[turn], block[...]))
        work[:, :size] = gram_parts(parts)
        work[:, size:] = eye
        inverse_factor(work, size)
        right_ref[...] = left_ref[...]
        basis = right_apply(parts, work[:, size:])
        block[...] = basis
        left_ref[...] = basis
        return carry

    left_ref[...] = start_ref[...]
    lax.fori_loop(0, 2 * sweeps, step, 0)
    image = apply_parts(both_high[1], both_low[1], right_ref[...])
    mass_ref[...] = exact(left_ref[...], image, ((0,), (0,)))


def subspace_bases(cross_gram, start_block):
    rank, size = start_block.shape
    tall_shape = jax.ShapeDtypeStruct((rank, size), jnp.float32)
    vmem = pl.BlockSpec(memory_space=pltpu.VMEM)
    return pl.pallas_call(
        functools.partial(bases_kernel, 2),
        out_shape=(tall_shape, tall_shape, jax.ShapeDtypeStruct((size, size), jnp.float32)),
        in_specs=[vmem, vmem],
        out_specs=(vmem, vmem, vmem),
        scratch_shapes=[
            pltpu.VMEM((2, rank, rank), jnp.bfloat16),
            pltpu.VMEM((2, rank, rank), jnp.bfloat16),
            pltpu.VMEM((rank, size), jnp.float32),
            pltpu.VMEM((size, 2 * size), jnp.float32),
        ],
    )(cross_gram, start_block)


def block_order(k, count, per_plane):
    inner = jnp.where(k < 2 * per_plane, count - 2 * per_plane + k, k - per_plane)
    return jnp.where(k < per_plane, k, inner)


def project_kernel(nslab, nsub, per_plane, *refs):
    ctrl_cells, obs_cells, right_ref, left_ref, ctrl_ref, obs_ref = refs[:6]
    faces, halves, landed, (send, recv) = refs[6:10], refs[10], refs[11:15], refs[15:]
    k = pl.program_id(0)
    count = pl.num_programs(0) // 2
    planes, lines, points, size = ctrl_ref.shape
    slab, sub = lax.axis_index("slab"), lax.axis_index("sub")
    moves = (
        ("slab", slab, nslab, 1, ctrl_ref.at[planes - 1]),
        ("slab", slab, nslab, -1, ctrl_ref.at[0]),
        ("sub", sub, nsub, 1, ctrl_ref.at[:, lines - 1]),
        ("sub", sub, nsub, -1, ctrl_ref.at[:, 0]),
    )

    def there(me, total, step):
        return me < total - 1 if step > 0 else me > 0

    def copy(m):
        axis, me, _, step, source = moves[m]
        return pltpu.make_async_remote_copy(
            src_ref=source,
            dst_ref=landed[m],
            send_sem=send.at[m],
            recv_sem=recv.at[m],
            device_id={axis: me + step},
        )

    def each(picked, act):
        for m in picked:
            _, me, total, step, _ = moves[m]

            @pl.when(there(me, total, step))
            def _():
                act(m)

    def product(cells, which):
        high, low = two_parts(cells)
        wide = narrow(high, halves[which])
        return wide[:, :size] + (wide[:, size:] + narrow(low, halves[which, :, :size]))

    @pl.when(k == 0)
    def _():
        barrier = pltpu.get_barrier_semaphore()
        for axis, me, total, step, _ in moves:
            beside = lax.rem(me + step + total, total)
            pl.semaphore_signal(barrier, inc=1, device_id={axis: beside})
        pl.semaphore_wait(barrier, len(moves))
        for which, basis in enumerate((right_ref, left_ref)):
            high, low = two_parts(basis[...])
            halves[which, :, :size] = high
            halves[which, :, size:] = low

    @pl.when(k < count)
    def _():
        block = block_order(k, count, per_plane)
        some = lines // per_plane
        value = product(ctrl_cells[...], 0).reshape(some, points, size)
        ctrl_ref[block // per_plane, pl.ds(lax.rem(block, per_plane) * some, some)] = value

    @pl.when(k >= count)
    def _():
        obs_ref[...] = product(obs_cells[...], 1)

    @pl.when(k == 2 * per_plane - 1)
    def _():
        each((0, 1), lambda m: copy(m).start())

    @pl.when(k == count - 1)
    def _():
        each((2, 3), lambda m: copy(m).start())

    @pl.when(k == 2 * count - 1)
    def _():
        for m, (_, me, total, step, _) in enumerate(moves):

            @pl.when(there(me, total, step))
            def _():
                copy(m).wait_send()

            @pl.when(there(me, total, -step))
            def _():
                copy(m).wait_recv()
                faces[m][...] = landed[m][...]

            @pl.when(jnp.logical_not(there(me, total, -step)))
            def _():
                faces[m][...] = jnp.zeros(landed[m].shape, jnp.float32)


def project(factor_ctrl, factor_obs, right_basis, left_basis, ident):
    nslab, nsub = lax.axis_size("slab"), lax.axis_size("sub")
    planes, lines, points, wide = factor_ctrl.shape
    cells, size = planes * lines * points, right_basis.shape[1]
    per_plane = 2 if lines % 2 == 0 else 1
    count, step = planes * per_plane, lines * points // per_plane
    shapes = [(lines, points, size)] * 2 + [(planes, points, size)] * 2
    grid_shape = (planes, lines, points, size)
    four = pltpu.SemaphoreType.DMA((4,))
    basis_spec = pl.BlockSpec((wide, size), lambda k: (0, 0))
    return pl.pallas_call(
        functools.partial(project_kernel, nslab, nsub, per_plane),
        grid=(2 * count,),
        out_shape=[
            jax.ShapeDtypeStruct(grid_shape, jnp.float32),
            jax.ShapeDtypeStruct((cells, size), jnp.float32),
        ]
        + [jax.ShapeDtypeStruct(shape, jnp.float32) for shape in shapes],
        in_specs=[
            pl.BlockSpec(
                (step, wide),
                lambda k: (block_order(jnp.minimum(k, count - 1), count, per_plane), 0),
            ),
            pl.BlockSpec((step, wide), lambda k: (jnp.maximum(k - count, 0), 0)),
            basis_spec,
            basis_spec,
        ],
        out_specs=[
            pl.BlockSpec(grid_shape, lambda k: (0, 0, 0, 0)),
            pl.BlockSpec((step, size), lambda k: (jnp.maximum(k - count, 0), 0)),
        ]
        + [pl.BlockSpec(shape, lambda k: (0, 0, 0)) for shape in shapes],
        scratch_shapes=[pltpu.VMEM((2, wide, 2 * size), jnp.bfloat16)]
        + [pltpu.VMEM(shape, jnp.float32) for shape in shapes]
        + [four, four],
        compiler_params=pltpu.CompilerParams(
            collective_id=ident,
            has_side_effects=True,
            dimension_semantics=("arbitrary",),
        ),
    )(factor_ctrl.reshape(cells, wide), factor_obs.reshape(cells, wide), right_basis, left_basis)


def on_device(factor_obs, factor_ctrl, diffusivity, input_map, output_map, start_block, order):
    planes, lines, points, rank = factor_ctrl.shape
    cells = planes * lines * points
    size = start_block.shape[1]
    observe = factor_obs.reshape(cells, rank)
    control = factor_ctrl.reshape(cells, rank)
    conduct = diffusivity.reshape(planes, lines, points)
    drive = input_map.reshape(input_map.shape[0], cells)
    sense = output_map.reshape(output_map.shape[0], cells)
    ins, outs = drive.shape[0], sense.shape[0]

    cross_gram = all_reduce(gram(observe, control), 0)
    left_basis, right_basis, mass = subspace_bases(cross_gram, start_block)

    ctrl, obs_space, below, above, before, after = project(
        factor_ctrl, factor_obs, right_basis, left_basis, 2
    )
    ctrl_flat = ctrl.reshape(cells, size)
    below, above = below[None], above[None]
    before, after = before[:, None], after[:, None]
    zs = jnp.concatenate([below, ctrl, above], axis=0)
    ys = jnp.concatenate([before, ctrl, after], axis=1)
    xs = jnp.pad(ctrl, ((0, 0), (0, 0), (1, 1), (0, 0)))
    beside = zs[2:] + zs[:-2] + ys[:, 2:] + ys[:, :-2] + xs[:, :, 2:] + xs[:, :, :-2]
    applied = (conduct[..., None] * (beside - 6.0 * ctrl) / 6.0).reshape(cells, size)
    state = tall(obs_space, applied, ((0,), (0,)))
    used = size + ins + outs
    grain = 8 * lax.axis_size("slab")
    packed = jnp.concatenate(
        [
            state,
            tall(drive, obs_space),
            tall(sense, ctrl_flat),
            jnp.zeros((-used % grain, size), jnp.float32),
        ],
        axis=0,
    )
    summed = small_all_reduce(packed, 1)
    kept = (jnp.arange(size, dtype=jnp.int32) < order[0]).astype(jnp.float32)
    square = kept[:, None] * kept[None, :]
    reduced_input = kept[:, None] * summed[size : size + ins].T
    reduced_output = kept[None, :] * summed[size + ins : used]
    return (square * mass, square * summed[:size], reduced_input, reduced_output)


def solution(mesh):
    placed = (
        P("slab", "sub", None, None),
        P("slab", "sub", None, None),
        P("slab", "sub"),
        P(None, "slab", "sub"),
        P(None, "slab", "sub"),
        P(),
        P(),
    )
    return jax.shard_map(
        on_device, mesh=mesh, in_specs=placed, out_specs=(P(), P(), P(), P()), check_vma=False
    )
```

```python
import functools
import jax
import jax.numpy as jnp
from jax import lax
from jax.experimental import pallas as pl
from jax.experimental.pallas import tpu as pltpu
from jax.sharding import PartitionSpec as P

LANES = 128
SUBS = 8
PANEL = 16
VMEM_BYTES = 60 * 1024 * 1024
HIGHEST = lax.Precision.HIGHEST


def exact(first, second, dims=((1,), (0,))):
    return lax.dot_general(
        first, second, (dims, ((), ())), precision=HIGHEST, preferred_element_type=jnp.float32
    )


def narrow(first, second, dims=((1,), (0,))):
    return lax.dot_general(first, second, (dims, ((), ())), preferred_element_type=jnp.float32)


def three_parts(value):
    high = value.astype(jnp.bfloat16).astype(jnp.float32)
    mid = (value - high).astype(jnp.bfloat16).astype(jnp.float32)
    return high, mid, value - high - mid


def two_parts(value):
    high = value.astype(jnp.bfloat16)
    return high, (value - high.astype(jnp.float32)).astype(jnp.bfloat16)


def three_dots(first, second, dims=((1,), (0,))):
    (a, b), (c, d) = two_parts(first), two_parts(second)
    return narrow(a, c, dims) + (narrow(a, d, dims) + narrow(b, c, dims))


def sub_bits(count):
    return [1 << b for b in range(count.bit_length() - 1)]


def across(block, sub):
    return jnp.broadcast_to(block[sub : sub + 1, :], block.shape)

def column(rows, lane):
    return jnp.broadcast_to(rows[:, lane : lane + 1], (SUBS, LANES))

def inverse_factor(work, size):
    wide = 2 * size // LANES
    place = lax.broadcasted_iota(jnp.int32, (SUBS, 2 * size), 0)
    spread = lambda x: jnp.concatenate([x] * wide, axis=1)
    carried = [work[h * SUBS : (h + 1) * SUBS, :] for h in range(2)]
    for base in range(0, size, PANEL):
        low, high = carried
        cols_low = [column(low, base + j) for j in range(SUBS)]
        cols_high = [column(high, base + j) for j in range(PANEL)]
        panel_low, panel_high = low, high
        scales, rows, leads = [], [], []
        for j in range(PANEL):
            if j < SUBS:
                scale = lax.rsqrt(across(cols_low[j], j))
                lead_low = cols_low[j] * scale
                row = across(low, j) * spread(scale)
                panel_low = jnp.where(place == j, row, panel_low)
            else:
                scale = lax.rsqrt(across(cols_high[j], j - SUBS))
                row = across(high, j - SUBS) * spread(scale)
                panel_high = jnp.where(place == j - SUBS, row, panel_high)
            lead_high = cols_high[j] * scale
            lead = {}
            for m in range(j + 1, PANEL):
                if m < SUBS:
                    lead[m] = across(lead_low, m)
                    cols_low[m] = cols_low[m] - lead_low * lead[m]
                else:
                    lead[m] = across(lead_high, m - SUBS)
                cols_high[m] = cols_high[m] - lead_high * lead[m]
            if j < SUBS - 1:
                low = low - spread(lead_low) * row
            if j < PANEL - 1:
                high = high - spread(lead_high) * row
            scales.append(scale)
            rows.append(row)
            leads.append(lead)
        panel = jnp.concatenate([panel_low, panel_high], axis=0)
        work[base : base + PANEL, :] = panel
        if base + PANEL < size:
            start = base + PANEL
            carried = []
            for h in range(2):
                rest = work[start + h * SUBS : start + (h + 1) * SUBS, :]
                cols = [column(rest, base + j) for j in range(PANEL)]
                for j in range(PANEL):
                    lead_rest = cols[j] * scales[j]
                    for m in range(j + 1, PANEL):
                        cols[m] = cols[m] - lead_rest * leads[j][m]
                    rest = rest - spread(lead_rest) * rows[j]
                carried.append(rest)
        if base + 2 * PANEL < size:
            start = base + 2 * PANEL
            high, mid, low = three_parts(panel)
            first = jnp.concatenate([high, high, mid, high, low, mid], axis=0)[:, :size]
            second = jnp.concatenate([high, mid, high, low, high, mid], axis=0)
            update = narrow(first.astype(jnp.bfloat16), second.astype(jnp.bfloat16), ((0,), (0,)))
            work[start:, :] = work[start:, :] - update[start:, :]


def pair(value):
    return jnp.concatenate(two_parts(value), axis=1)


def fold(wide, size):
    return wide[:, :size] + wide[:, size:]


def apply_parts(high, low, block):
    size = block.shape[1]
    parts = pair(block)
    return fold(narrow(high, parts) + narrow(low, parts), size)


def gram_parts(parts):
    size = parts.shape[1] // 2
    full = narrow(parts, parts, ((0,), (0,)))
    return (full[:size, :size] + full[size:, size:]) + (full[:size, size:] + full[size:, :size])


def right_apply(parts, factor):
    turned = pair(factor.T)
    return fold(narrow(parts, jnp.concatenate([turned, turned], axis=0)), factor.shape[0])


def far_count(nslab):
    return max(nslab // 2, 1)


def front_kernel(nslab, nsub, points, *refs):
    obs_hbm, ctrl_hbm, conduct_ref, drive_ref, sense_ref = refs[:5]
    gram_ref, inner_ref, maps_ref = refs[5:8]
    obs, ctrl, spread_k, applied_high, applied_low, acc, work, got, got_far, load = refs[8:18]
    rs_send, rs_recv, far_send, far_recv, back_send, back_recv, ag_send, ag_recv = refs[18:]
    slab, sub = lax.axis_index("slab"), lax.axis_index("sub")
    cells, wide = ctrl.shape
    planes, plane_cells = conduct_ref.shape
    step = applied_high.shape[0]
    count = cells // step
    nfar = far_count(nslab)
    turns = [("sub", bit) for bit in sub_bits(nsub)] + [("slab", 1)]
    orders = (turns, turns[:1] + turns[1:][::-1])

    def fetch(which, k):
        rows = pl.ds(k * step, step)
        source, target = ((obs_hbm, obs), (ctrl_hbm, ctrl))[which]
        return pltpu.make_async_copy(source.at[rows], target.at[rows], load.at[which, k])

    for k in range(count):
        fetch(0, k).start()
        fetch(1, k).start()

    def partner(axis, bit):
        index = slab if axis == "slab" else sub
        has = lax.rem(index // bit, 2)
        return has, {axis: index + bit - 2 * bit * has}

    def far(off):
        other = lax.rem(slab // 2 + off, nfar)
        return other, {"slab": other * 2 + lax.rem(slab, 2)}

    barrier = pltpu.get_barrier_semaphore()
    for axis, bit in turns:
        pl.semaphore_signal(barrier, inc=1, device_id=partner(axis, bit)[1])
    for off in range(1, nfar):
        pl.semaphore_signal(barrier, inc=1, device_id=far(off)[1])

    for p in range(planes):
        for c in range(plane_cells // LANES):
            lanes = conduct_ref[p : p + 1, c * LANES : (c + 1) * LANES] * (1.0 / 6.0)
            first = p * plane_cells + c * LANES
            spread_k[first : first + LANES, :] = jnp.broadcast_to(lanes, (LANES, LANES)).T
    acc[...] = jnp.zeros_like(acc)

    def add_block(k, carry):
        fetch(0, k).wait()
        fetch(1, k).wait()
        rows = pl.ds(pl.multiple_of(k * step, step), step)
        acc[...] += three_dots(obs[rows, :], ctrl[rows, :], ((0,), (0,)))
        return carry

    lax.fori_loop(0, count, add_block, 0)
    tall_rows = acc.shape[0]
    for c in range(acc.shape[1] // LANES):
        work[c * tall_rows : (c + 1) * tall_rows, :] = acc[:, c * LANES : (c + 1) * LANES]
    pl.semaphore_wait(barrier, len(turns) + nfar - 1)

    place = lax.broadcasted_iota(jnp.int32, (points, wide), 0)

    def inner_block(k):
        first = k * step
        plane = first // plane_cells

        def line(i, carry):
            row = pl.multiple_of(first + i * points, points)
            within = lax.rem(row, plane_cells)
            here = ctrl[pl.ds(row, points), :]
            total = jnp.where(place > 0, pltpu.roll(here, 1, 0), 0.0)
            total = total + jnp.where(place < points - 1, pltpu.roll(here, points - 1, 0), 0.0)
            before = pl.multiple_of(jnp.maximum(row - points, 0), points)
            after = pl.multiple_of(jnp.minimum(row + points, cells - points), points)
            total = total + jnp.where(within > 0, 1.0, 0.0) * ctrl[pl.ds(before, points), :]
            inside = jnp.where(within < plane_cells - points, 1.0, 0.0)
            total = total + inside * ctrl[pl.ds(after, points), :]
            if plane > 0:
                total = total + ctrl[pl.ds(row - plane_cells, points), :]
            if plane < planes - 1:
                total = total + ctrl[pl.ds(row + plane_cells, points), :]
            scale = jnp.concatenate([spread_k[pl.ds(row, points), :]] * (wide // LANES), axis=1)
            high, low = two_parts(scale * (total - 6.0 * here))
            applied_high[pl.ds(pl.multiple_of(i * points, points), points), :] = high
            applied_low[pl.ds(pl.multiple_of(i * points, points), points), :] = low
            return carry

        lax.fori_loop(0, step // points, line, 0)
        rows = slice(first, first + step)
        high, low = two_parts(obs[rows, :])
        dims = ((0,), (0,))
        value = narrow(high, applied_high[...], dims) + (
            narrow(high, applied_low[...], dims) + narrow(low, applied_high[...], dims)
        )
        lanes = slice(first % plane_cells, first % plane_cells + step)
        seen = three_dots(drive_ref[:, plane, lanes], obs[rows, :])
        felt = three_dots(sense_ref[:, plane, lanes], ctrl[rows, :])
        both = jnp.concatenate([seen, felt], axis=0)
        if k == 0:
            inner_ref[...] = value
            maps_ref[...] = both
        else:
            inner_ref[...] += value
            maps_ref[...] += both

    blocks = iter(range(count))

    def work_meanwhile(amount):
        for _ in range(amount):
            k = next(blocks, None)
            if k is not None:
                inner_block(k)

    gaps = 2 * len(turns) + 2
    share = -(-count // gaps)
    rows = work.shape[0]
    length = rows // 2
    bases, taken = [0, length], 0
    for s in range(len(turns)):
        length = length // 2
        copies, keeps = [], []
        for h in range(2):
            axis, bit = orders[h][s]
            has, target = partner(axis, bit)
            keeps.append(pl.multiple_of(bases[h] + has * length, 8))
            give = pl.multiple_of(bases[h] + (1 - has) * length, 8)
            copies.append(
                pltpu.make_async_remote_copy(
                    src_ref=work.at[pl.ds(give, length)],
                    dst_ref=got.at[h, pl.ds(taken, length)],
                    send_sem=rs_send.at[h, s],
                    recv_sem=rs_recv.at[h, s],
                    device_id=target,
                )
            )
            copies[h].start()
        work_meanwhile(share)
        for h in range(2):
            copies[h].wait()
            work[pl.ds(keeps[h], length), :] += got[h, taken : taken + length, :]
        bases, taken = keeps, taken + length

    piece = length // nfar
    mines = [pl.multiple_of(bases[h] + (slab // 2) * piece, 8) for h in range(2)]
    copies = []
    for h in range(2):
        for off in range(1, nfar):
            other, target = far(off)
            copy = pltpu.make_async_remote_copy(
                src_ref=work.at[pl.ds(pl.multiple_of(bases[h] + other * piece, 8), piece)],
                dst_ref=got_far.at[h, off],
                send_sem=far_send.at[h, off],
                recv_sem=far_recv.at[h, off],
                device_id=target,
            )
            copy.start()
            copies.append(copy)
    work_meanwhile(share)
    for copy in copies:
        copy.wait()
    for h in range(2):
        total = work[pl.ds(mines[h], piece), :]
        for off in range(1, nfar):
            total = total + got_far[h, off]
        gram_ref[pl.ds(mines[h], piece), :] = total

    copies = []
    for h in range(2):
        for off in range(1, nfar):
            copy = pltpu.make_async_remote_copy(
                src_ref=gram_ref.at[pl.ds(mines[h], piece)],
                dst_ref=gram_ref.at[pl.ds(mines[h], piece)],
                send_sem=back_send.at[h, off],
                recv_sem=back_recv.at[h, off],
                device_id=far(off)[1],
            )
            copy.start()
            copies.append(copy)
    work_meanwhile(share)
    for copy in copies:
        copy.wait()

    for s in reversed(range(len(turns))):
        copies, nexts = [], []
        for h in range(2):
            axis, bit = orders[h][s]
            has, target = partner(axis, bit)
            copy = pltpu.make_async_remote_copy(
                src_ref=gram_ref.at[pl.ds(bases[h], length)],
                dst_ref=gram_ref.at[pl.ds(bases[h], length)],
                send_sem=ag_send.at[h, s],
                recv_sem=ag_recv.at[h, s],
                device_id=target,
            )
            copy.start()
            copies.append(copy)
            nexts.append(pl.multiple_of(bases[h] - has * length, 8))
        work_meanwhile(share if s else count)
        for copy in copies:
            copy.wait()
        bases, length = nexts, 2 * length


def front(factor_obs, factor_ctrl, diffusivity, input_map, output_map, ident):
    nslab, nsub = lax.axis_size("slab"), lax.axis_size("sub")
    planes, lines, points, wide = factor_ctrl.shape
    cells = planes * lines * points
    step = lines * points // (2 if lines % 2 == 0 else 1)
    rows = wide * (wide // LANES)
    nfar, turns = far_count(nslab), len(sub_bits(nsub)) + 1
    half = rows // 2
    maps = input_map.shape[0] + output_map.shape[0]
    vmem, anywhere = pl.BlockSpec(memory_space=pltpu.VMEM), pl.BlockSpec(memory_space=pl.ANY)
    near, far = pltpu.SemaphoreType.DMA((2, turns)), pltpu.SemaphoreType.DMA((2, nfar))
    f32, bf16 = jnp.float32, jnp.bfloat16
    return pl.pallas_call(
        functools.partial(front_kernel, nslab, nsub, points),
        out_shape=[
            jax.ShapeDtypeStruct((rows, LANES), f32),
            jax.ShapeDtypeStruct((wide, wide), f32),
            jax.ShapeDtypeStruct((maps, wide), f32),
        ],
        in_specs=[anywhere, anywhere, vmem, vmem, vmem],
        out_specs=[vmem, vmem, vmem],
        scratch_shapes=[
            pltpu.VMEM((cells, wide), f32),
            pltpu.VMEM((cells, wide), f32),
            pltpu.VMEM((cells, LANES), f32),
            pltpu.VMEM((step, wide), bf16),
            pltpu.VMEM((step, wide), bf16),
            pltpu.VMEM((wide, wide), f32),
            pltpu.VMEM((rows, LANES), f32),
            pltpu.VMEM((2, half, LANES), f32),
            pltpu.VMEM((2, nfar, half // 2**turns // nfar, LANES), f32),
            pltpu.SemaphoreType.DMA((2, cells // step)),
            near, near, far, far, far, far, near, near,
        ],
        compiler_params=pltpu.CompilerParams(
            collective_id=ident, has_side_effects=True, vmem_limit_bytes=VMEM_BYTES
        ),
    )(
        factor_obs.reshape(cells, wide),
        factor_ctrl.reshape(cells, wide),
        diffusivity,
        input_map,
        output_map,
    )


def face_chunks(cells):
    return 2 if cells % 16 == 0 else 1


def back_kernel(nslab, nsub, points, sweeps, *refs):
    order_ref, gram_ref, start_ref, inner_ref, maps_ref, conduct_ref, obs_hbm, ctrl_hbm = refs[:8]
    mass_ref, state_ref, in_ref, out_ref = refs[8:12]
    both_high, both_low, block, left_ref, right_ref, work, turned, face = refs[12:20]
    obs_z, obs_y, ctrl_z, ctrl_y, send_z, send_y, got_z, got_y = refs[20:28]
    flat, pack, slots, result = refs[28:32]
    load, z_send, z_recv, y_send, y_recv, rs_send, rs_recv, ag_send, ag_recv = refs[32:]
    slab, sub = lax.axis_index("slab"), lax.axis_index("sub")
    rank, size = start_ref.shape
    planes, plane_cells = conduct_ref.shape
    total, me = nslab * nsub, slab * nsub + sub
    chunks = face_chunks(plane_cells)
    chunk = plane_cells // chunks

    def peer(off):
        other = lax.rem(me + off, total)
        return other, {"slab": other // nsub, "sub": lax.rem(other, nsub)}

    barrier = pltpu.get_barrier_semaphore()

    def greet(off, carry):
        pl.semaphore_signal(barrier, inc=1, device_id=peer(off)[1])
        return carry

    lax.fori_loop(1, total, greet, 0)

    loads = []
    for which, (source, z_face, y_face) in enumerate(
        ((ctrl_hbm, ctrl_z, ctrl_y), (obs_hbm, obs_z, obs_y))
    ):
        for side in range(2):
            plane = side * (planes - 1)
            pairs = [(source.at[pl.ds(plane * plane_cells, plane_cells)], z_face.at[side])]
            for p in range(planes):
                first = p * plane_cells + side * (plane_cells - points)
                pairs.append(
                    (source.at[pl.ds(first, points)], y_face.at[side, pl.ds(p * points, points)])
                )
            for i, (here, there) in enumerate(pairs):
                loads.append(pltpu.make_async_copy(here, there, load.at[which, side, i]))
    for copy in loads:
        copy.start()

    for c in range(rank // LANES):
        cols = slice(c * LANES, (c + 1) * LANES)
        tile = gram_ref[c * rank : (c + 1) * rank, :]
        high, low = two_parts(tile)
        both_high[1, :, cols] = high
        both_low[1, :, cols] = low
        high, low = two_parts(tile.T)
        both_high[0, cols, :] = high
        both_low[0, cols, :] = low
    block[...] = start_ref[...]
    row = lax.broadcasted_iota(jnp.int32, (size, size), 0)
    col = lax.broadcasted_iota(jnp.int32, (size, size), 1)
    eye = (row == col).astype(jnp.float32)
    pl.semaphore_wait(barrier, total - 1)

    places = (("slab", slab, nslab, 1), ("slab", slab, nslab, -1))
    places = places + (("sub", sub, nsub, 1), ("sub", sub, nsub, -1))

    def beside(m, way):
        _, index, count, step = places[m]
        return index < count - 1 if step * way > 0 else index > 0

    def copy_z(m, c):
        axis, index, _, step = places[m]
        return pltpu.make_async_remote_copy(
            src_ref=send_z.at[m, c],
            dst_ref=got_z.at[m, c],
            send_sem=z_send.at[m, c],
            recv_sem=z_recv.at[m, c],
            device_id={axis: index + step},
        )

    def copy_y(m):
        axis, index, _, step = places[2 + m]
        return pltpu.make_async_remote_copy(
            src_ref=send_y.at[m],
            dst_ref=got_y.at[m],
            send_sem=y_send.at[m],
            recv_sem=y_recv.at[m],
            device_id={axis: index + step},
        )

    def project(cells, parts):
        high, low = two_parts(cells)
        return fold(narrow(high, parts) + narrow(low, parts), size)

    def send_faces():
        parts = pair(apply_parts(both_high[1], both_low[1], block[...]))
        image = narrow(both_high[0], parts) + narrow(both_low[0], parts)
        parts = pair(fold(image, size))
        for copy in loads[: len(loads) // 2]:
            copy.wait()
        for c in range(chunks):
            for m in range(2):
                rows = slice(c * chunk, (c + 1) * chunk)
                send_z[m, c] = project(ctrl_z[1 - m, rows, :], parts)

                @pl.when(beside(m, 1))
                def _():
                    copy_z(m, c).start()

        for m in range(2):
            send_y[m] = project(ctrl_y[1 - m], parts)

            @pl.when(beside(2 + m, 1))
            def _():
                copy_y(m).start()

    def step(k, carry):
        turn = lax.rem(k, 2)
        parts = pair(apply_parts(both_high[turn], both_low[turn], block[...]))
        work[:, :size] = gram_parts(parts)
        work[:, size:] = eye
        inverse_factor(work, size)
        right_ref[...] = left_ref[...]
        basis = right_apply(parts, work[:, size:])
        block[...] = basis
        left_ref[...] = basis

        @pl.when(k == 2 * sweeps - 4)
        def _():
            send_faces()
            turned[...] = eye

        @pl.when(jnp.logical_and(k > 2 * sweeps - 4, k < 2 * sweeps - 1))
        def _():
            turned[...] = exact(turned[...], work[:, size:], ((1,), (1,)))

        return carry

    left_ref[...] = start_ref[...]
    lax.fori_loop(0, 2 * sweeps, step, 0)

    left_parts, right_parts = pair(left_ref[...]), pair(right_ref[...])
    image = fold(narrow(both_high[1], right_parts) + narrow(both_low[1], right_parts), size)
    kept = order_ref[0]
    square = jnp.where(jnp.logical_and(row < kept, col < kept), 1.0, 0.0)
    mass_ref[...] = square * exact(left_ref[...], image, ((0,), (0,)))
    state = exact(left_ref[...], project(inner_ref[...], right_parts), ((0,), (0,)))
    maps = maps_ref.shape[0]
    ins = in_ref.shape[1]
    seen = project(maps_ref[...], left_parts)
    felt = project(maps_ref[...], right_parts)
    side = lax.broadcasted_iota(jnp.int32, seen.shape, 0)
    flat[...] = jnp.zeros_like(flat)
    flat[size : size + maps, :] = jnp.where(side < ins, seen, felt)
    for copy in loads[len(loads) // 2 :]:
        copy.wait()

    def spread(plane, group):
        lanes = conduct_ref[plane : plane + 1, group * LANES : (group + 1) * LANES] * (1.0 / 6.0)
        return jnp.broadcast_to(lanes, (LANES, LANES)).T

    groups = plane_cells // LANES
    face[...] = jnp.zeros_like(face)
    for m in range(2):
        mine = project(obs_y[m], left_parts)
        last = [spread(p, m * (groups - 1)) for p in range(planes)]
        scale = [part[LANES - points :] if m else part[:points] for part in last]
        mine = mine * jnp.concatenate(scale, axis=0)

        @pl.when(beside(2 + m, -1))
        def _():
            copy_y(m).wait_recv()
            face[...] += three_dots(mine, got_y[m], ((0,), (0,)))

    for c in range(chunks):
        for m in range(2):
            rows = slice(c * chunk, (c + 1) * chunk)
            mine = project(obs_z[m, rows, :], left_parts)
            per = groups // chunks
            scale = [spread(m * (planes - 1), c * per + g) for g in range(per)]
            mine = mine * jnp.concatenate(scale, axis=0)

            @pl.when(beside(m, -1))
            def _():
                copy_z(m, c).wait_recv()
                face[...] += three_dots(mine, got_z[m, c], ((0,), (0,)))

    flat[:size, :] = state + exact(face[...], turned[...])
    part = pack.shape[1]
    owners = -(-(size + maps) // part)
    pack[...] = jnp.zeros_like(pack)
    for d in range(owners):
        pack[d] = flat[d * part : (d + 1) * part, :]

    def gather(off):
        other, target = peer(off)
        return pltpu.make_async_remote_copy(
            src_ref=pack.at[other],
            dst_ref=slots.at[off],
            send_sem=rs_send.at[off],
            recv_sem=rs_recv.at[off],
            device_id=target,
        )

    def spread_out(off):
        return pltpu.make_async_remote_copy(
            src_ref=result.at[me],
            dst_ref=result.at[me],
            send_sem=ag_send.at[off],
            recv_sem=ag_recv.at[off],
            device_id=peer(off)[1],
        )

    def loop(act):
        def body(off, carry):
            act(off)
            return carry

        lax.fori_loop(1, total, body, 0)

    loop(lambda off: gather(off).start())
    slots[0] = pack[me]
    loop(lambda off: gather(off).wait())
    result[me] = jnp.sum(slots[...], axis=0)
    loop(lambda off: spread_out(off).start())
    for m in range(2):

        @pl.when(beside(2 + m, 1))
        def _():
            copy_y(m).wait_send()

        for c in range(chunks):

            @pl.when(beside(m, 1))
            def _():
                copy_z(m, c).wait_send()

    loop(lambda off: spread_out(off).wait())
    for d in range(owners):
        flat[d * part : (d + 1) * part, :] = result[d]
    state_ref[...] = square * flat[:size, :]
    lanes = jnp.where(col[:maps, :] < kept, 1.0, 0.0) * flat[size : size + maps, :]
    in_ref[...] = lanes.T[:, :ins]
    out_ref[...] = lanes[ins:, :]


def back(order, gram, start, inner, maps, diffusivity, factor_obs, factor_ctrl, ins, ident):
    nslab, nsub = lax.axis_size("slab"), lax.axis_size("sub")
    planes, lines, points, wide = factor_ctrl.shape
    cells, plane_cells = planes * lines * points, lines * points
    rank, size = start.shape
    total = nslab * nsub
    rows = size + maps.shape[0]
    part = -(-rows // total)
    chunks = face_chunks(plane_cells)
    side = planes * points
    f32, bf16 = jnp.float32, jnp.bfloat16
    vmem, anywhere = pl.BlockSpec(memory_space=pltpu.VMEM), pl.BlockSpec(memory_space=pl.ANY)
    every = pltpu.SemaphoreType.DMA((total,))
    zs, ys = pltpu.SemaphoreType.DMA((2, chunks)), pltpu.SemaphoreType.DMA((2,))
    faces_z = pltpu.VMEM((2, chunks, plane_cells // chunks, size), f32)
    faces_y = pltpu.VMEM((2, side, size), f32)
    return pl.pallas_call(
        functools.partial(back_kernel, nslab, nsub, points, 2),
        out_shape=[
            jax.ShapeDtypeStruct((size, size), f32),
            jax.ShapeDtypeStruct((size, size), f32),
            jax.ShapeDtypeStruct((size, ins), f32),
            jax.ShapeDtypeStruct((maps.shape[0] - ins, size), f32),
        ],
        in_specs=[pl.BlockSpec(memory_space=pltpu.SMEM)] + [vmem] * 5 + [anywhere] * 2,
        out_specs=[vmem] * 4,
        scratch_shapes=[
            pltpu.VMEM((2, rank, rank), bf16),
            pltpu.VMEM((2, rank, rank), bf16),
            pltpu.VMEM((rank, size), f32),
            pltpu.VMEM((rank, size), f32),
            pltpu.VMEM((rank, size), f32),
            pltpu.VMEM((size, 2 * size), f32),
            pltpu.VMEM((size, size), f32),
            pltpu.VMEM((size, size), f32),
            pltpu.VMEM((2, plane_cells, wide), f32),
            pltpu.VMEM((2, side, wide), f32),
            pltpu.VMEM((2, plane_cells, wide), f32),
            pltpu.VMEM((2, side, wide), f32),
            faces_z, faces_y, faces_z, faces_y,
            pltpu.VMEM((part * -(-rows // part), LANES), f32),
            pltpu.VMEM((total, part, LANES), f32),
            pltpu.VMEM((total, part, LANES), f32),
            pltpu.VMEM((total, part, LANES), f32),
            pltpu.SemaphoreType.DMA((2, 2, planes + 1)),
            zs, zs, ys, ys, every, every, every, every,
        ],
        compiler_params=pltpu.CompilerParams(
            collective_id=ident, has_side_effects=True, vmem_limit_bytes=VMEM_BYTES
        ),
    )(
        order,
        gram,
        start,
        inner,
        maps,
        diffusivity,
        factor_obs.reshape(cells, wide),
        factor_ctrl.reshape(cells, wide),
    )


def on_device(factor_obs, factor_ctrl, diffusivity, input_map, output_map, start_block, order):
    gram, inner, maps = front(factor_obs, factor_ctrl, diffusivity, input_map, output_map, 0)
    ins = input_map.shape[0]
    return tuple(
        back(order, gram, start_block, inner, maps, diffusivity, factor_obs, factor_ctrl, ins, 1)
    )


def solution(mesh):
    placed = (
        P("slab", "sub", None, None),
        P("slab", "sub", None, None),
        P("slab", "sub"),
        P(None, "slab", "sub"),
        P(None, "slab", "sub"),
        P(),
        P(),
    )
    return jax.shard_map(
        on_device, mesh=mesh, in_specs=placed, out_specs=(P(), P(), P(), P()), check_vma=False
    )
```

```python
import functools
import jax
import jax.numpy as jnp
from jax import lax
from jax.experimental import pallas as pl
from jax.experimental.pallas import tpu as pltpu
from jax.sharding import PartitionSpec as P

LANES = 128
SUBS = 8
PANEL = 16
VMEM_BYTES = 60 * 1024 * 1024
HIGHEST = lax.Precision.HIGHEST


def exact(first, second, dims=((1,), (0,))):
    return lax.dot_general(
        first, second, (dims, ((), ())), precision=HIGHEST, preferred_element_type=jnp.float32
    )


def narrow(first, second, dims=((1,), (0,))):
    return lax.dot_general(first, second, (dims, ((), ())), preferred_element_type=jnp.float32)


def three_parts(value):
    high = value.astype(jnp.bfloat16).astype(jnp.float32)
    mid = (value - high).astype(jnp.bfloat16).astype(jnp.float32)
    return high, mid, value - high - mid


def two_parts(value):
    high = value.astype(jnp.bfloat16)
    return high, (value - high.astype(jnp.float32)).astype(jnp.bfloat16)


def three_dots(first, second, dims=((1,), (0,))):
    (a, b), (c, d) = two_parts(first), two_parts(second)
    return narrow(a, c, dims) + (narrow(a, d, dims) + narrow(b, c, dims))


def sub_bits(count):
    return [1 << b for b in range(count.bit_length() - 1)]


def far_count(nslab):
    return max(nslab // 2, 1)


def face_chunks(cells):
    return 2 if cells % 16 == 0 else 1


def across(block, sub):
    return jnp.broadcast_to(block[sub : sub + 1, :], block.shape)

def column(rows, lane):
    return jnp.broadcast_to(rows[:, lane : lane + 1], (SUBS, LANES))

def inverse_factor(work, size):
    wide = 2 * size // LANES
    place = lax.broadcasted_iota(jnp.int32, (SUBS, 2 * size), 0)
    spread = lambda x: jnp.concatenate([x] * wide, axis=1)
    carried = [work[h * SUBS : (h + 1) * SUBS, :] for h in range(2)]
    for base in range(0, size, PANEL):
        low, high = carried
        cols_low = [column(low, base + j) for j in range(SUBS)]
        cols_high = [column(high, base + j) for j in range(PANEL)]
        panel_low, panel_high = low, high
        scales, rows, leads = [], [], []
        for j in range(PANEL):
            if j < SUBS:
                scale = lax.rsqrt(across(cols_low[j], j))
                lead_low = cols_low[j] * scale
                row = across(low, j) * spread(scale)
                panel_low = jnp.where(place == j, row, panel_low)
            else:
                scale = lax.rsqrt(across(cols_high[j], j - SUBS))
                row = across(high, j - SUBS) * spread(scale)
                panel_high = jnp.where(place == j - SUBS, row, panel_high)
            lead_high = cols_high[j] * scale
            lead = {}
            for m in range(j + 1, PANEL):
                if m < SUBS:
                    lead[m] = across(lead_low, m)
                    cols_low[m] = cols_low[m] - lead_low * lead[m]
                else:
                    lead[m] = across(lead_high, m - SUBS)
                cols_high[m] = cols_high[m] - lead_high * lead[m]
            if j < SUBS - 1:
                low = low - spread(lead_low) * row
            if j < PANEL - 1:
                high = high - spread(lead_high) * row
            scales.append(scale)
            rows.append(row)
            leads.append(lead)
        panel = jnp.concatenate([panel_low, panel_high], axis=0)
        work[base : base + PANEL, :] = panel
        if base + PANEL < size:
            start = base + PANEL
            carried = []
            for h in range(2):
                rest = work[start + h * SUBS : start + (h + 1) * SUBS, :]
                cols = [column(rest, base + j) for j in range(PANEL)]
                for j in range(PANEL):
                    lead_rest = cols[j] * scales[j]
                    for m in range(j + 1, PANEL):
                        cols[m] = cols[m] - lead_rest * leads[j][m]
                    rest = rest - spread(lead_rest) * rows[j]
                carried.append(rest)
        if base + 2 * PANEL < size:
            start = base + 2 * PANEL
            high, mid, low = three_parts(panel)
            first = jnp.concatenate([high, high, mid, high, low, mid], axis=0)[:, :size]
            second = jnp.concatenate([high, mid, high, low, high, mid], axis=0)
            update = narrow(first.astype(jnp.bfloat16), second.astype(jnp.bfloat16), ((0,), (0,)))
            work[start:, :] = work[start:, :] - update[start:, :]


def pair(value):
    return jnp.concatenate(two_parts(value), axis=1)


def fold(wide, size):
    return wide[:, :size] + wide[:, size:]


def apply_parts(high, low, block):
    size = block.shape[1]
    parts = pair(block)
    return fold(narrow(high, parts) + narrow(low, parts), size)


def gram_parts(parts):
    size = parts.shape[1] // 2
    full = narrow(parts, parts, ((0,), (0,)))
    return (full[:size, :size] + full[size:, size:]) + (full[:size, size:] + full[size:, :size])


def right_apply(parts, factor):
    turned = pair(factor.T)
    return fold(narrow(parts, jnp.concatenate([turned, turned], axis=0)), factor.shape[0])


def peers(slab, sub, nslab, nsub):
    everyone, me = nslab * nsub, slab * nsub + sub

    def peer(off):
        other = lax.rem(me + off, everyone)
        return other, {"slab": other // nsub, "sub": lax.rem(other, nsub)}

    return everyone, me, peer


def whole_kernel(nslab, nsub, points, sweeps, *refs):
    obs_hbm, ctrl_hbm, conduct_hbm, drive_hbm, sense_hbm, start_hbm, out_ref = refs[:7]
    obs, ctrl, conduct, drive, sense, start, spread_k, applied_high, applied_low = refs[7:16]
    acc, inner, maps, work, got, got_far, whole = refs[16:23]
    both_high, both_low, left, right, square, turned, face = refs[23:30]
    send_z, send_y, got_z, got_y, pack, slots, result = refs[30:37]
    load, load_small = refs[37:39]
    rs_send, rs_recv, far_send, far_recv, back_send, back_recv, ag_send, ag_recv = refs[39:47]
    z_send, z_recv, y_send, y_recv, sum_send, sum_recv, give_send, give_recv = refs[47:]
    slab, sub = lax.axis_index("slab"), lax.axis_index("sub")
    everyone, me, peer = peers(slab, sub, nslab, nsub)
    cells, wide = ctrl.shape
    planes, plane_cells = conduct.shape
    step = applied_high.shape[0]
    count = cells // step
    nfar = far_count(nslab)
    turns = [("sub", bit) for bit in sub_bits(nsub)] + [("slab", 1)]
    orders = (turns, turns[:1] + turns[1:][::-1])

    def fetch(which, k):
        rows = pl.ds(k * step, step)
        source, target = ((obs_hbm, obs), (ctrl_hbm, ctrl))[which]
        return pltpu.make_async_copy(source.at[rows], target.at[rows], load.at[which, k])

    small = [
        pltpu.make_async_copy(here, there, load_small.at[i])
        for i, (here, there) in enumerate(
            ((conduct_hbm, conduct), (drive_hbm, drive), (sense_hbm, sense), (start_hbm, start))
        )
    ]
    small[0].start()
    for k in range(count):
        fetch(0, k).start()
        fetch(1, k).start()
    for copy in small[1:]:
        copy.start()

    def partner(axis, bit):
        index = slab if axis == "slab" else sub
        has = lax.rem(index // bit, 2)
        return has, {axis: index + bit - 2 * bit * has}

    def far(off):
        other = lax.rem(slab // 2 + off, nfar)
        return other, {"slab": other * 2 + lax.rem(slab, 2)}

    barrier = pltpu.get_barrier_semaphore()

    def greet(off, carry):
        pl.semaphore_signal(barrier, inc=1, device_id=peer(off)[1])
        return carry

    lax.fori_loop(1, everyone, greet, 0)
    small[0].wait()
    for p in range(planes):
        for c in range(plane_cells // LANES):
            lanes = conduct[p : p + 1, c * LANES : (c + 1) * LANES] * (1.0 / 6.0)
            first = p * plane_cells + c * LANES
            spread_k[first : first + LANES, :] = jnp.broadcast_to(lanes, (LANES, LANES)).T
    acc[...] = jnp.zeros_like(acc)

    def add_block(k, carry):
        fetch(0, k).wait()
        fetch(1, k).wait()
        rows = pl.ds(pl.multiple_of(k * step, step), step)
        acc[...] += three_dots(obs[rows, :], ctrl[rows, :], ((0,), (0,)))
        return carry

    lax.fori_loop(0, count, add_block, 0)
    tall_rows = acc.shape[0]
    for c in range(acc.shape[1] // LANES):
        work[c * tall_rows : (c + 1) * tall_rows, :] = acc[:, c * LANES : (c + 1) * LANES]
    for copy in small[1:]:
        copy.wait()
    pl.semaphore_wait(barrier, everyone - 1)

    place = lax.broadcasted_iota(jnp.int32, (points, wide), 0)

    def inner_block(k):
        first = k * step
        plane = first // plane_cells

        def line(i, carry):
            row = pl.multiple_of(first + i * points, points)
            within = lax.rem(row, plane_cells)
            here = ctrl[pl.ds(row, points), :]
            total = jnp.where(place > 0, pltpu.roll(here, 1, 0), 0.0)
            total = total + jnp.where(place < points - 1, pltpu.roll(here, points - 1, 0), 0.0)
            before = pl.multiple_of(jnp.maximum(row - points, 0), points)
            after = pl.multiple_of(jnp.minimum(row + points, cells - points), points)
            total = total + jnp.where(within > 0, 1.0, 0.0) * ctrl[pl.ds(before, points), :]
            inside = jnp.where(within < plane_cells - points, 1.0, 0.0)
            total = total + inside * ctrl[pl.ds(after, points), :]
            if plane > 0:
                total = total + ctrl[pl.ds(row - plane_cells, points), :]
            if plane < planes - 1:
                total = total + ctrl[pl.ds(row + plane_cells, points), :]
            scale = jnp.concatenate([spread_k[pl.ds(row, points), :]] * (wide // LANES), axis=1)
            high, low = two_parts(scale * (total - 6.0 * here))
            applied_high[pl.ds(pl.multiple_of(i * points, points), points), :] = high
            applied_low[pl.ds(pl.multiple_of(i * points, points), points), :] = low
            return carry

        lax.fori_loop(0, step // points, line, 0)
        rows = slice(first, first + step)
        high, low = two_parts(obs[rows, :])
        dims = ((0,), (0,))
        value = narrow(high, applied_high[...], dims) + (
            narrow(high, applied_low[...], dims) + narrow(low, applied_high[...], dims)
        )
        lanes = slice(first % plane_cells, first % plane_cells + step)
        seen = three_dots(drive[:, plane, lanes], obs[rows, :])
        felt = three_dots(sense[:, plane, lanes], ctrl[rows, :])
        both = jnp.concatenate([seen, felt], axis=0)
        if k == 0:
            inner[...] = value
            maps[...] = both
        else:
            inner[...] += value
            maps[...] += both

    blocks = iter(range(count))

    def work_meanwhile(amount):
        for _ in range(amount):
            k = next(blocks, None)
            if k is not None:
                inner_block(k)

    gaps = 2 * len(turns) + 2
    share = -(-count // gaps)
    rows = work.shape[0]
    length = rows // 2
    bases, taken = [0, length], 0
    for s in range(len(turns)):
        length = length // 2
        copies, keeps = [], []
        for h in range(2):
            axis, bit = orders[h][s]
            has, target = partner(axis, bit)
            keeps.append(pl.multiple_of(bases[h] + has * length, 8))
            give = pl.multiple_of(bases[h] + (1 - has) * length, 8)
            copies.append(
                pltpu.make_async_remote_copy(
                    src_ref=work.at[pl.ds(give, length)],
                    dst_ref=got.at[h, pl.ds(taken, length)],
                    send_sem=rs_send.at[h, s],
                    recv_sem=rs_recv.at[h, s],
                    device_id=target,
                )
            )
            copies[h].start()
        work_meanwhile(share)
        for h in range(2):
            copies[h].wait()
            work[pl.ds(keeps[h], length), :] += got[h, taken : taken + length, :]
        bases, taken = keeps, taken + length

    piece = length // nfar
    mines = [pl.multiple_of(bases[h] + (slab // 2) * piece, 8) for h in range(2)]
    copies = []
    for h in range(2):
        for off in range(1, nfar):
            other, target = far(off)
            copy = pltpu.make_async_remote_copy(
                src_ref=work.at[pl.ds(pl.multiple_of(bases[h] + other * piece, 8), piece)],
                dst_ref=got_far.at[h, off],
                send_sem=far_send.at[h, off],
                recv_sem=far_recv.at[h, off],
                device_id=target,
            )
            copy.start()
            copies.append(copy)
    work_meanwhile(share)
    for copy in copies:
        copy.wait()
    for h in range(2):
        total = work[pl.ds(mines[h], piece), :]
        for off in range(1, nfar):
            total = total + got_far[h, off]
        whole[pl.ds(mines[h], piece), :] = total

    copies = []
    for h in range(2):
        for off in range(1, nfar):
            copy = pltpu.make_async_remote_copy(
                src_ref=whole.at[pl.ds(mines[h], piece)],
                dst_ref=whole.at[pl.ds(mines[h], piece)],
                send_sem=back_send.at[h, off],
                recv_sem=back_recv.at[h, off],
                device_id=far(off)[1],
            )
            copy.start()
            copies.append(copy)
    work_meanwhile(share)
    for copy in copies:
        copy.wait()

    for s in reversed(range(len(turns))):
        copies, nexts = [], []
        for h in range(2):
            axis, bit = orders[h][s]
            has, target = partner(axis, bit)
            copy = pltpu.make_async_remote_copy(
                src_ref=whole.at[pl.ds(bases[h], length)],
                dst_ref=whole.at[pl.ds(bases[h], length)],
                send_sem=ag_send.at[h, s],
                recv_sem=ag_recv.at[h, s],
                device_id=target,
            )
            copy.start()
            copies.append(copy)
            nexts.append(pl.multiple_of(bases[h] - has * length, 8))
        work_meanwhile(share if s else count)
        for copy in copies:
            copy.wait()
        bases, length = nexts, 2 * length

    rank, size = start.shape
    chunks = face_chunks(plane_cells)
    chunk = plane_cells // chunks

    def edge_lines(ref, side):
        firsts = [p * plane_cells + side * (plane_cells - points) for p in range(planes)]
        return jnp.concatenate([ref[first : first + points, :] for first in firsts], axis=0)

    for c in range(rank // LANES):
        cols = slice(c * LANES, (c + 1) * LANES)
        tile = whole[c * rank : (c + 1) * rank, :]
        high, low = two_parts(tile)
        both_high[1, :, cols] = high
        both_low[1, :, cols] = low
        high, low = two_parts(tile.T)
        both_high[0, cols, :] = high
        both_low[0, cols, :] = low
    row = lax.broadcasted_iota(jnp.int32, (size, size), 0)
    col = lax.broadcasted_iota(jnp.int32, (size, size), 1)
    eye = (row == col).astype(jnp.float32)

    places = (("slab", slab, nslab, 1), ("slab", slab, nslab, -1))
    places = places + (("sub", sub, nsub, 1), ("sub", sub, nsub, -1))

    def beside(m, way):
        _, index, count, step = places[m]
        return index < count - 1 if step * way > 0 else index > 0

    def copy_z(m, c):
        axis, index, _, step = places[m]
        return pltpu.make_async_remote_copy(
            src_ref=send_z.at[m, c],
            dst_ref=got_z.at[m, c],
            send_sem=z_send.at[m, c],
            recv_sem=z_recv.at[m, c],
            device_id={axis: index + step},
        )

    def copy_y(m):
        axis, index, _, step = places[2 + m]
        return pltpu.make_async_remote_copy(
            src_ref=send_y.at[m],
            dst_ref=got_y.at[m],
            send_sem=y_send.at[m],
            recv_sem=y_recv.at[m],
            device_id={axis: index + step},
        )

    def project(cells, parts):
        high, low = two_parts(cells)
        return fold(narrow(high, parts) + narrow(low, parts), size)

    def send_faces():
        parts = pair(apply_parts(both_high[1], both_low[1], left[...]))
        image = narrow(both_high[0], parts) + narrow(both_low[0], parts)
        parts = pair(fold(image, size))
        for c in range(chunks):
            for m in range(2):
                first = (1 - m) * (planes - 1) * plane_cells + c * chunk
                send_z[m, c] = project(ctrl[first : first + chunk, :], parts)

                @pl.when(beside(m, 1))
                def _():
                    copy_z(m, c).start()

        for m in range(2):
            send_y[m] = project(edge_lines(ctrl, 1 - m), parts)

            @pl.when(beside(2 + m, 1))
            def _():
                copy_y(m).start()

    def sweep(k, carry):
        turn = lax.rem(k, 2)
        parts = pair(apply_parts(both_high[turn], both_low[turn], left[...]))
        square[:, :size] = gram_parts(parts)
        square[:, size:] = eye
        inverse_factor(square, size)
        right[...] = left[...]
        basis = right_apply(parts, square[:, size:])
        left[...] = basis

        @pl.when(k == 2 * sweeps - 4)
        def _():
            send_faces()
            turned[...] = eye

        @pl.when(jnp.logical_and(k > 2 * sweeps - 4, k < 2 * sweeps - 1))
        def _():
            turned[...] = exact(turned[...], square[:, size:], ((1,), (1,)))

        return carry

    left[...] = start[...]
    lax.fori_loop(0, 2 * sweeps, sweep, 0)

    left_parts, right_parts = pair(left[...]), pair(right[...])
    image = fold(narrow(both_high[1], right_parts) + narrow(both_low[1], right_parts), size)
    out_ref[:size, :] = exact(left[...], image, ((0,), (0,)))
    state = exact(left[...], project(inner[...], right_parts), ((0,), (0,)))
    ins, both_maps = drive.shape[0], maps.shape[0]
    seen = project(maps[...], left_parts)
    felt = project(maps[...], right_parts)
    side = lax.broadcasted_iota(jnp.int32, seen.shape, 0)
    out_ref[2 * size :, :] = jnp.zeros((out_ref.shape[0] - 2 * size, size), jnp.float32)
    out_ref[2 * size : 2 * size + both_maps, :] = jnp.where(side < ins, seen, felt)

    face[...] = jnp.zeros_like(face)
    for m in range(2):
        mine = project(edge_lines(obs, m), left_parts) * edge_lines(spread_k, m)

        @pl.when(beside(2 + m, -1))
        def _():
            copy_y(m).wait_recv()
            face[...] += three_dots(mine, got_y[m], ((0,), (0,)))

    for c in range(chunks):
        for m in range(2):
            first = m * (planes - 1) * plane_cells + c * chunk
            rows = slice(first, first + chunk)
            mine = project(obs[rows, :], left_parts) * spread_k[rows, :]

            @pl.when(beside(m, -1))
            def _():
                copy_z(m, c).wait_recv()
                face[...] += three_dots(mine, got_z[m, c], ((0,), (0,)))

    out_ref[size : 2 * size, :] = state + exact(face[...], turned[...])
    part = pack.shape[1]
    owners = (out_ref.shape[0] - size) // part
    pack[...] = jnp.zeros_like(pack)
    for d in range(owners):
        pack[d] = out_ref[size + d * part : size + (d + 1) * part, :]

    def gather(off):
        other, target = peer(off)
        return pltpu.make_async_remote_copy(
            src_ref=pack.at[other],
            dst_ref=slots.at[off],
            send_sem=sum_send.at[off],
            recv_sem=sum_recv.at[off],
            device_id=target,
        )

    def spread_out(off):
        return pltpu.make_async_remote_copy(
            src_ref=result.at[me],
            dst_ref=result.at[me],
            send_sem=give_send.at[off],
            recv_sem=give_recv.at[off],
            device_id=peer(off)[1],
        )

    def loop(act):
        def body(off, carry):
            act(off)
            return carry

        lax.fori_loop(1, everyone, body, 0)

    loop(lambda off: gather(off).start())
    slots[0] = pack[me]
    loop(lambda off: gather(off).wait())
    result[me] = jnp.sum(slots[...], axis=0)
    loop(lambda off: spread_out(off).start())
    for m in range(2):

        @pl.when(beside(2 + m, 1))
        def _():
            copy_y(m).wait_send()

        for c in range(chunks):

            @pl.when(beside(m, 1))
            def _():
                copy_z(m, c).wait_send()

    loop(lambda off: spread_out(off).wait())
    for d in range(owners):
        out_ref[size + d * part : size + (d + 1) * part, :] = result[d]


def finish_kernel(order_ref, raw_ref, mass_ref, state_ref, in_ref, out_ref):
    size, ins = in_ref.shape
    outs = out_ref.shape[0]
    kept = order_ref[0]
    row = lax.broadcasted_iota(jnp.int32, (size, size), 0)
    col = lax.broadcasted_iota(jnp.int32, (size, size), 1)
    square = jnp.where(jnp.logical_and(row < kept, col < kept), 1.0, 0.0)
    mass_ref[...] = square * raw_ref[:size, :]
    state_ref[...] = square * raw_ref[size : 2 * size, :]
    lanes = jnp.where(col[: ins + outs, :] < kept, 1.0, 0.0)
    lanes = lanes * raw_ref[2 * size : 2 * size + ins + outs, :]
    in_ref[...] = lanes.T[:, :ins]
    out_ref[...] = lanes[ins:, :]


def on_device(factor_obs, factor_ctrl, diffusivity, input_map, output_map, start_block, order):
    nslab, nsub = lax.axis_size("slab"), lax.axis_size("sub")
    planes, lines, points, wide = factor_ctrl.shape
    cells, plane_cells = planes * lines * points, lines * points
    rank, size = start_block.shape
    ins, outs = input_map.shape[0], output_map.shape[0]
    everyone = nslab * nsub
    step = plane_cells // (2 if lines % 2 == 0 else 1)
    rows = wide * (wide // LANES)
    half = rows // 2
    nfar, turns = far_count(nslab), len(sub_bits(nsub)) + 1
    part = -(-(size + ins + outs) // everyone)
    owners = -(-(size + ins + outs) // part)
    chunks = face_chunks(plane_cells)
    side = planes * points
    f32, bf16 = jnp.float32, jnp.bfloat16
    vmem, anywhere = pl.BlockSpec(memory_space=pltpu.VMEM), pl.BlockSpec(memory_space=pl.ANY)
    near, far = pltpu.SemaphoreType.DMA((2, turns)), pltpu.SemaphoreType.DMA((2, nfar))
    every = pltpu.SemaphoreType.DMA((everyone,))
    zs, ys = pltpu.SemaphoreType.DMA((2, chunks)), pltpu.SemaphoreType.DMA((2,))
    faces_z = pltpu.VMEM((2, chunks, plane_cells // chunks, size), f32)
    faces_y = pltpu.VMEM((2, side, size), f32)
    pieces = pltpu.VMEM((everyone, part, LANES), f32)
    raw = pl.pallas_call(
        functools.partial(whole_kernel, nslab, nsub, points, 2),
        out_shape=jax.ShapeDtypeStruct((size + owners * part, size), f32),
        in_specs=[anywhere] * 6,
        out_specs=vmem,
        scratch_shapes=[
            pltpu.VMEM((cells, wide), f32),
            pltpu.VMEM((cells, wide), f32),
            pltpu.VMEM((planes, plane_cells), f32),
            pltpu.VMEM(input_map.shape, f32),
            pltpu.VMEM(output_map.shape, f32),
            pltpu.VMEM((rank, size), f32),
            pltpu.VMEM((cells, LANES), f32),
            pltpu.VMEM((step, wide), bf16),
            pltpu.VMEM((step, wide), bf16),
            pltpu.VMEM((wide, wide), f32),
            pltpu.VMEM((wide, wide), f32),
            pltpu.VMEM((ins + outs, wide), f32),
            pltpu.VMEM((rows, LANES), f32),
            pltpu.VMEM((2, half, LANES), f32),
            pltpu.VMEM((2, nfar, half // 2**turns // nfar, LANES), f32),
            pltpu.VMEM((rows, LANES), f32),
            pltpu.VMEM((2, rank, rank), bf16),
            pltpu.VMEM((2, rank, rank), bf16),
            pltpu.VMEM((rank, size), f32),
            pltpu.VMEM((rank, size), f32),
            pltpu.VMEM((size, 2 * size), f32),
            pltpu.VMEM((size, size), f32),
            pltpu.VMEM((size, size), f32),
            faces_z, faces_y, faces_z, faces_y, pieces, pieces, pieces,
            pltpu.SemaphoreType.DMA((2, cells // step)),
            pltpu.SemaphoreType.DMA((4,)),
            near, near, far, far, far, far, near, near,
            zs, zs, ys, ys, every, every, every, every,
        ],
        compiler_params=pltpu.CompilerParams(
            collective_id=0, has_side_effects=True, vmem_limit_bytes=VMEM_BYTES
        ),
    )(
        factor_obs.reshape(cells, wide),
        factor_ctrl.reshape(cells, wide),
        diffusivity,
        input_map,
        output_map,
        start_block,
    )
    return tuple(
        pl.pallas_call(
            finish_kernel,
            out_shape=[
                jax.ShapeDtypeStruct((size, size), f32),
                jax.ShapeDtypeStruct((size, size), f32),
                jax.ShapeDtypeStruct((size, ins), f32),
                jax.ShapeDtypeStruct((outs, size), f32),
            ],
            in_specs=[pl.BlockSpec(memory_space=pltpu.SMEM), vmem],
            out_specs=[vmem] * 4,
        )(order, raw)
    )


def solution(mesh):
    placed = (
        P("slab", "sub", None, None),
        P("slab", "sub", None, None),
        P("slab", "sub"),
        P(None, "slab", "sub"),
        P(None, "slab", "sub"),
        P(),
        P(),
    )
    return jax.shard_map(
        on_device, mesh=mesh, in_specs=placed, out_specs=(P(), P(), P(), P()), check_vma=False
    )
```

```python
import functools
import jax
import jax.numpy as jnp
from jax import lax
from jax.experimental import pallas as pl
from jax.experimental.pallas import tpu as pltpu
from jax.sharding import PartitionSpec as P

LANES = 128
SUBS = 8
PANEL = 16
VMEM_BYTES = 60 * 1024 * 1024
EARLY_LINES = 2
HIGHEST = lax.Precision.HIGHEST


def exact(first, second, dims=((1,), (0,))):
    return lax.dot_general(
        first, second, (dims, ((), ())), precision=HIGHEST, preferred_element_type=jnp.float32
    )


def narrow(first, second, dims=((1,), (0,))):
    return lax.dot_general(first, second, (dims, ((), ())), preferred_element_type=jnp.float32)


def three_parts(value):
    high = value.astype(jnp.bfloat16).astype(jnp.float32)
    mid = (value - high).astype(jnp.bfloat16).astype(jnp.float32)
    return high, mid, value - high - mid


def two_parts(value):
    high = value.astype(jnp.bfloat16)
    return high, (value - high.astype(jnp.float32)).astype(jnp.bfloat16)


def three_dots(first, second, dims=((1,), (0,))):
    (a, b), (c, d) = two_parts(first), two_parts(second)
    return narrow(a, c, dims) + (narrow(a, d, dims) + narrow(b, c, dims))


def sub_bits(count):
    return [1 << b for b in range(count.bit_length() - 1)]


def far_count(nslab):
    return max(nslab // 2, 1)


def face_chunks(cells):
    return 2 if cells % 16 == 0 else 1


def across(block, sub):
    return jnp.broadcast_to(block[sub : sub + 1, :], block.shape)

def column(rows, lane):
    return jnp.broadcast_to(rows[:, lane : lane + 1], (SUBS, LANES))

def inverse_factor(work, size):
    wide = 2 * size // LANES
    place = lax.broadcasted_iota(jnp.int32, (SUBS, 2 * size), 0)
    spread = lambda x: jnp.concatenate([x] * wide, axis=1)
    carried = [work[h * SUBS : (h + 1) * SUBS, :] for h in range(2)]
    for base in range(0, size, PANEL):
        low, high = carried
        cols_low = [column(low, base + j) for j in range(SUBS)]
        cols_high = [column(high, base + j) for j in range(PANEL)]
        panel_low, panel_high = low, high
        scales, rows, leads = [], [], []
        for j in range(PANEL):
            if j < SUBS:
                scale = lax.rsqrt(across(cols_low[j], j))
                lead_low = cols_low[j] * scale
                row = across(low, j) * spread(scale)
                panel_low = jnp.where(place == j, row, panel_low)
            else:
                scale = lax.rsqrt(across(cols_high[j], j - SUBS))
                row = across(high, j - SUBS) * spread(scale)
                panel_high = jnp.where(place == j - SUBS, row, panel_high)
            lead_high = cols_high[j] * scale
            lead = {}
            for m in range(j + 1, PANEL):
                if m < SUBS:
                    lead[m] = across(lead_low, m)
                    cols_low[m] = cols_low[m] - lead_low * lead[m]
                else:
                    lead[m] = across(lead_high, m - SUBS)
                cols_high[m] = cols_high[m] - lead_high * lead[m]
            if j < SUBS - 1:
                low = low - spread(lead_low) * row
            if j < PANEL - 1:
                high = high - spread(lead_high) * row
            scales.append(scale)
            rows.append(row)
            leads.append(lead)
        panel = jnp.concatenate([panel_low, panel_high], axis=0)
        work[base : base + PANEL, :] = panel
        if base + PANEL < size:
            start = base + PANEL
            carried = []
            for h in range(2):
                rest = work[start + h * SUBS : start + (h + 1) * SUBS, :]
                cols = [column(rest, base + j) for j in range(PANEL)]
                for j in range(PANEL):
                    lead_rest = cols[j] * scales[j]
                    for m in range(j + 1, PANEL):
                        cols[m] = cols[m] - lead_rest * leads[j][m]
                    rest = rest - spread(lead_rest) * rows[j]
                carried.append(rest)
        if base + 2 * PANEL < size:
            start = base + 2 * PANEL
            high, mid, low = three_parts(panel)
            first = jnp.concatenate([high, high, mid, high, low, mid], axis=0)[:, :size]
            second = jnp.concatenate([high, mid, high, low, high, mid], axis=0)
            update = narrow(first.astype(jnp.bfloat16), second.astype(jnp.bfloat16), ((0,), (0,)))
            work[start:, :] = work[start:, :] - update[start:, :]


def pair(value):
    return jnp.concatenate(two_parts(value), axis=1)


def fold(wide, size):
    return wide[:, :size] + wide[:, size:]


def apply_parts(high, low, block):
    size = block.shape[1]
    parts = pair(block)
    return fold(narrow(high, parts) + narrow(low, parts), size)


def gram_parts(parts):
    size = parts.shape[1] // 2
    full = narrow(parts, parts, ((0,), (0,)))
    return (full[:size, :size] + full[size:, size:]) + (full[:size, size:] + full[size:, :size])


def right_apply(parts, factor):
    turned = pair(factor.T)
    return fold(narrow(parts, jnp.concatenate([turned, turned], axis=0)), factor.shape[0])


def peers(slab, sub, nslab, nsub):
    everyone, me = nslab * nsub, slab * nsub + sub

    def peer(off):
        other = lax.rem(me + off, everyone)
        return other, {"slab": other // nsub, "sub": lax.rem(other, nsub)}

    return everyone, me, peer


def whole_kernel(nslab, nsub, points, sweeps, *refs):
    obs_hbm, ctrl_hbm, conduct_hbm, drive_hbm, sense_hbm, start_hbm, out_ref = refs[:7]
    obs, ctrl, conduct, drive, sense, start, spread_k, applied_high, applied_low = refs[7:16]
    turns = [("sub", bit) for bit in sub_bits(nsub)] + [("slab", 1)]
    refs = list(refs[16:])

    def take(count):
        return [refs.pop(0) for _ in range(count)]

    acc, inner, maps, work, whole, got_far = take(6)
    got = take(len(turns))
    both_high, both_low, left, right, square, turned, face = take(7)
    send_z, send_y, got_z, got_y, pack, slots, result = take(7)
    raw_z, load, load_small, raw_send, raw_recv = take(5)
    rs_send, rs_recv, far_send, far_recv, back_send, back_recv, ag_send, ag_recv = take(8)
    z_send, z_recv, y_send, y_recv, sum_send, sum_recv, give_send, give_recv = take(8)
    slab, sub = lax.axis_index("slab"), lax.axis_index("sub")
    everyone, me, peer = peers(slab, sub, nslab, nsub)
    cells, wide = ctrl.shape
    planes, plane_cells = conduct.shape
    step = applied_high.shape[0]
    count = cells // step
    nfar = far_count(nslab)

    def fetch(which, k):
        rows = pl.ds(k * step, step)
        source, target = ((obs_hbm, obs), (ctrl_hbm, ctrl))[which]
        return pltpu.make_async_copy(source.at[rows], target.at[rows], load.at[which, k])

    places = (("slab", slab, nslab, 1), ("slab", slab, nslab, -1))
    places = places + (("sub", sub, nsub, 1), ("sub", sub, nsub, -1))

    def beside(m, way):
        _, index, count, step = places[m]
        return index < count - 1 if step * way > 0 else index > 0

    def copy_raw(m):
        axis, index, _, way = places[m]
        first = (1 - m) * (planes - 1) * plane_cells
        return pltpu.make_async_remote_copy(
            src_ref=ctrl_hbm.at[pl.ds(first, raw_z.shape[1])],
            dst_ref=raw_z.at[m],
            send_sem=raw_send.at[m],
            recv_sem=raw_recv.at[m],
            device_id={axis: index + way},
        )

    small = [
        pltpu.make_async_copy(here, there, load_small.at[i])
        for i, (here, there) in enumerate(
            ((conduct_hbm, conduct), (drive_hbm, drive), (sense_hbm, sense), (start_hbm, start))
        )
    ]
    small[0].start()
    ahead = min(2, count)
    for k in range(ahead):
        fetch(0, k).start()
        fetch(1, k).start()
    for copy in small[1:]:
        copy.start()

    def partner(axis, bit):
        index = slab if axis == "slab" else sub
        has = lax.rem(index // bit, 2)
        return has, {axis: index + bit - 2 * bit * has}

    def far(off):
        other = lax.rem(slab // 2 + off, nfar)
        return other, {"slab": other * 2 + lax.rem(slab, 2)}

    barrier = pltpu.get_barrier_semaphore()

    def greet(off, carry):
        pl.semaphore_signal(barrier, inc=1, device_id=peer(off)[1])
        return carry

    lax.fori_loop(1, everyone, greet, 0)
    small[0].wait()
    for p in range(planes):
        for c in range(plane_cells // LANES):
            lanes = conduct[p : p + 1, c * LANES : (c + 1) * LANES] * (1.0 / 6.0)
            first = p * plane_cells + c * LANES
            spread_k[first : first + LANES, :] = jnp.broadcast_to(lanes, (LANES, LANES)).T
    acc[...] = jnp.zeros_like(acc)

    def add_block(k, carry):
        fetch(0, k).wait()
        fetch(1, k).wait()

        @pl.when(k + ahead < count)
        def _():
            fetch(0, k + ahead).start()
            fetch(1, k + ahead).start()

        rows = pl.ds(pl.multiple_of(k * step, step), step)
        acc[...] += three_dots(ctrl[rows, :], obs[rows, :], ((0,), (0,)))
        return carry

    lax.fori_loop(0, 1, add_block, 0)
    pl.semaphore_wait(barrier, everyone - 1)
    for m in range(2):

        @pl.when(beside(m, 1))
        def _():
            copy_raw(m).start()

        @pl.when(jnp.logical_not(beside(m, -1)))
        def _():
            raw_z[m] = jnp.zeros(raw_z.shape[1:], jnp.float32)

    lax.fori_loop(1, count, add_block, 0)
    blocked = work.shape[1:]
    for c in range(acc.shape[1] // LANES):
        work[c] = acc[:, c * LANES : (c + 1) * LANES].reshape(blocked)
    for copy in small[1:]:
        copy.wait()

    place = lax.broadcasted_iota(jnp.int32, (points, wide), 0)

    def inner_block(k):
        first = k * step
        plane = first // plane_cells

        ends = ((0, 0), (1, planes - 1))
        sides = [m for m, at in ends if at == plane and first % plane_cells == 0]
        for m in sides:

            @pl.when(beside(m, -1))
            def _():
                copy_raw(m).wait_recv()

        def line(i, carry, sides=()):
            row = pl.multiple_of(first + i * points, points)
            within = lax.rem(row, plane_cells)
            here = ctrl[pl.ds(row, points), :]
            total = jnp.where(place > 0, pltpu.roll(here, 1, 0), 0.0)
            total = total + jnp.where(place < points - 1, pltpu.roll(here, points - 1, 0), 0.0)
            before = pl.multiple_of(jnp.maximum(row - points, 0), points)
            after = pl.multiple_of(jnp.minimum(row + points, cells - points), points)
            total = total + jnp.where(within > 0, 1.0, 0.0) * ctrl[pl.ds(before, points), :]
            inside = jnp.where(within < plane_cells - points, 1.0, 0.0)
            total = total + inside * ctrl[pl.ds(after, points), :]
            if plane > 0:
                total = total + ctrl[pl.ds(row - plane_cells, points), :]
            if plane < planes - 1:
                total = total + ctrl[pl.ds(row + plane_cells, points), :]
            for m in sides:
                total = total + raw_z[m, pl.ds(pl.multiple_of(i * points, points), points), :]
            scale = jnp.concatenate([spread_k[pl.ds(row, points), :]] * (wide // LANES), axis=1)
            high, low = two_parts(scale * (total - 6.0 * here))
            applied_high[pl.ds(pl.multiple_of(i * points, points), points), :] = high
            applied_low[pl.ds(pl.multiple_of(i * points, points), points), :] = low
            return carry

        extra = raw_z.shape[1] // points if sides else 0
        if sides:
            lax.fori_loop(0, extra, functools.partial(line, sides=sides), 0)
        lax.fori_loop(extra, step // points, line, 0)
        rows = slice(first, first + step)
        high, low = two_parts(obs[rows, :])
        dims = ((0,), (0,))
        value = narrow(high, applied_high[...], dims) + (
            narrow(high, applied_low[...], dims) + narrow(low, applied_high[...], dims)
        )
        lanes = slice(first % plane_cells, first % plane_cells + step)
        seen = three_dots(drive[:, plane, lanes], obs[rows, :])
        felt = three_dots(sense[:, plane, lanes], ctrl[rows, :])
        both = jnp.concatenate([seen, felt], axis=0)
        if k == sequence[0]:
            inner[...] = value
            maps[...] = both
        else:
            inner[...] += value
            maps[...] += both

    per_plane = plane_cells // step
    late = [0, (planes - 1) * per_plane]
    sequence = [k for k in range(count) if k not in late] + late
    blocks = iter(sequence)

    def work_meanwhile(amount):
        for _ in range(amount):
            k = next(blocks, None)
            if k is not None:
                inner_block(k)

    share = -(-count // (2 * len(turns) + 2))
    tiles = work.shape[0]
    here = [partner(axis, bit)[0] for axis, bit in turns]
    orders = [list(range(len(turns))) for _ in range(tiles)]
    for c in range(1, tiles, 2):
        orders[c] = orders[c][:1] + orders[c][1:][::-1]

    def region(c, done, flip=None):
        index = [slice(None)] * len(turns)
        for t in done:
            index[t] = here[t]
        if flip is not None:
            index[flip] = 1 - here[flip]
        return (c, *index)

    def halve(c, s):
        t = orders[c][s]
        return pltpu.make_async_remote_copy(
            src_ref=work.at[region(c, orders[c][:s], t)],
            dst_ref=got[s].at[c],
            send_sem=rs_send.at[c, s],
            recv_sem=rs_recv.at[c, s],
            device_id=partner(*turns[t])[1],
        )

    def scatter(c, off):
        other, target = far(off)
        return pltpu.make_async_remote_copy(
            src_ref=work.at[(c, *here, other)],
            dst_ref=got_far.at[c, off],
            send_sem=far_send.at[c, off],
            recv_sem=far_recv.at[c, off],
            device_id=target,
        )

    def gather_far(c, off):
        return pltpu.make_async_remote_copy(
            src_ref=whole.at[(c, *here, slab // 2)],
            dst_ref=whole.at[(c, *here, slab // 2)],
            send_sem=back_send.at[c, off],
            recv_sem=back_recv.at[c, off],
            device_id=far(off)[1],
        )

    def double(c, s):
        mine = region(c, orders[c][: s + 1])
        return pltpu.make_async_remote_copy(
            src_ref=whole.at[mine],
            dst_ref=whole.at[mine],
            send_sem=ag_send.at[c, s],
            recv_sem=ag_recv.at[c, s],
            device_id=partner(*turns[orders[c][s]])[1],
        )

    last = len(turns) - 1
    for s in range(len(turns)):
        for c in range(tiles):
            if s:
                halve(c, s - 1).wait()
                work[region(c, orders[c][:s])] += got[s - 1][c]
            halve(c, s).start()
        work_meanwhile(share)
    for c in range(tiles):
        halve(c, last).wait()
        work[(c, *here)] += got[last][c]
        for off in range(1, nfar):
            scatter(c, off).start()
    work_meanwhile(share)
    for c in range(tiles):
        total = work[(c, *here, slab // 2)]
        for off in range(1, nfar):
            scatter(c, off).wait()
            total = total + got_far[c, off]
        whole[(c, *here, slab // 2)] = total
        for off in range(1, nfar):
            gather_far(c, off).start()
    work_meanwhile(share)
    for s in reversed(range(len(turns))):
        for c in range(tiles):
            if s == last:
                for off in range(1, nfar):
                    gather_far(c, off).wait()
            else:
                double(c, s + 1).wait()
            double(c, s).start()
        work_meanwhile(share if s else count)
    for c in range(tiles):
        double(c, 0).wait()

    rank, size = start.shape
    chunks = face_chunks(plane_cells)
    early = raw_z.shape[1]
    chunk = (plane_cells - early) // chunks

    def edge_lines(ref, side):
        firsts = [p * plane_cells + side * (plane_cells - points) for p in range(planes)]
        return jnp.concatenate([ref[first : first + points, :] for first in firsts], axis=0)

    for c in range(tiles):
        cols = slice(c * LANES, (c + 1) * LANES)
        tile = whole[c].reshape(rank, LANES)
        high, low = two_parts(tile)
        both_high[0, :, cols] = high
        both_low[0, :, cols] = low
        high, low = two_parts(tile.T)
        both_high[1, cols, :] = high
        both_low[1, cols, :] = low
    left[...] = start[...]
    row = lax.broadcasted_iota(jnp.int32, (size, size), 0)
    col = lax.broadcasted_iota(jnp.int32, (size, size), 1)
    eye = (row == col).astype(jnp.float32)

    def copy_z(m, c):
        axis, index, _, step = places[m]
        return pltpu.make_async_remote_copy(
            src_ref=send_z.at[m, c],
            dst_ref=got_z.at[m, c],
            send_sem=z_send.at[m, c],
            recv_sem=z_recv.at[m, c],
            device_id={axis: index + step},
        )

    def copy_y(m):
        axis, index, _, step = places[2 + m]
        return pltpu.make_async_remote_copy(
            src_ref=send_y.at[m],
            dst_ref=got_y.at[m],
            send_sem=y_send.at[m],
            recv_sem=y_recv.at[m],
            device_id={axis: index + step},
        )

    def project(cells, parts):
        high, low = two_parts(cells)
        return fold(narrow(high, parts) + narrow(low, parts), size)

    def send_faces():
        parts = pair(apply_parts(both_high[1], both_low[1], left[...]))
        image = narrow(both_high[0], parts) + narrow(both_low[0], parts)
        parts = pair(fold(image, size))
        for c in range(chunks):
            for m in range(2):
                first = (1 - m) * (planes - 1) * plane_cells + early + c * chunk
                send_z[m, c] = project(ctrl[first : first + chunk, :], parts)

                @pl.when(beside(m, 1))
                def _():
                    copy_z(m, c).start()

        for m in range(2):
            send_y[m] = project(edge_lines(ctrl, 1 - m), parts)

            @pl.when(beside(2 + m, 1))
            def _():
                copy_y(m).start()

    def sweep(k, carry):
        turn = lax.rem(k, 2)
        parts = pair(apply_parts(both_high[turn], both_low[turn], left[...]))
        square[:, :size] = gram_parts(parts)
        square[:, size:] = eye
        inverse_factor(square, size)
        right[...] = left[...]
        basis = right_apply(parts, square[:, size:])
        left[...] = basis

        @pl.when(k == 2 * sweeps - 4)
        def _():
            send_faces()
            turned[...] = eye

        @pl.when(jnp.logical_and(k > 2 * sweeps - 4, k < 2 * sweeps - 1))
        def _():
            turned[...] = exact(turned[...], square[:, size:], ((1,), (1,)))

        return carry

    lax.fori_loop(0, 2 * sweeps, sweep, 0)

    left_parts, right_parts = pair(left[...]), pair(right[...])
    image = fold(narrow(both_high[1], right_parts) + narrow(both_low[1], right_parts), size)
    out_ref[:size, :] = exact(left[...], image, ((0,), (0,)))
    state = exact(left[...], project(inner[...], right_parts), ((0,), (0,)))
    ins, both_maps = drive.shape[0], maps.shape[0]
    seen = project(maps[...], left_parts)
    felt = project(maps[...], right_parts)
    side = lax.broadcasted_iota(jnp.int32, seen.shape, 0)
    out_ref[2 * size :, :] = jnp.zeros((out_ref.shape[0] - 2 * size, size), jnp.float32)
    out_ref[2 * size : 2 * size + both_maps, :] = jnp.where(side < ins, seen, felt)

    face[...] = jnp.zeros_like(face)
    for m in range(2):
        mine = project(edge_lines(obs, m), left_parts) * edge_lines(spread_k, m)

        @pl.when(beside(2 + m, -1))
        def _():
            copy_y(m).wait_recv()
            face[...] += three_dots(mine, got_y[m], ((0,), (0,)))

    for c in range(chunks):
        for m in range(2):
            first = m * (planes - 1) * plane_cells + early + c * chunk
            rows = slice(first, first + chunk)
            mine = project(obs[rows, :], left_parts) * spread_k[rows, :]

            @pl.when(beside(m, -1))
            def _():
                copy_z(m, c).wait_recv()
                face[...] += three_dots(mine, got_z[m, c], ((0,), (0,)))

    out_ref[size : 2 * size, :] = state + exact(face[...], turned[...])
    owners, part = pack.shape[:2]
    lead = (nslab // 4) * nsub
    rank_of = me - lead
    owning = jnp.logical_and(rank_of >= 0, rank_of < owners)
    for d in range(owners):
        pack[d] = out_ref[size + d * part : size + (d + 1) * part, :]

    def device(linear):
        return {"slab": linear // nsub, "sub": lax.rem(linear, nsub)}

    def collect(owner, source):
        return pltpu.make_async_remote_copy(
            src_ref=pack.at[owner],
            dst_ref=slots.at[source],
            send_sem=sum_send.at[owner],
            recv_sem=sum_recv.at[source],
            device_id=device(lead + owner),
        )

    def hand_out(owner, off):
        return pltpu.make_async_remote_copy(
            src_ref=result.at[owner],
            dst_ref=result.at[owner],
            send_sem=give_send.at[off],
            recv_sem=give_recv.at[owner],
            device_id=peer(off)[1],
        )

    def loop(start, stop, act):
        def body(i, carry):
            act(i)
            return carry

        lax.fori_loop(start, stop, body, 0)

    def unless_me(linear, act):
        @pl.when(linear != me)
        def _():
            act()

    loop(0, owners, lambda d: unless_me(lead + d, lambda: collect(d, me).start()))

    @pl.when(owning)
    def _():
        slots[me] = pack[rank_of]
        loop(0, everyone, lambda i: unless_me(i, lambda: collect(0, i).wait_recv()))
        result[rank_of] = jnp.sum(slots[...], axis=0)
        loop(1, everyone, lambda off: hand_out(rank_of, off).start())

    for m in range(2):

        @pl.when(beside(m, 1))
        def _():
            copy_raw(m).wait_send()

        @pl.when(beside(2 + m, 1))
        def _():
            copy_y(m).wait_send()

        for c in range(chunks):

            @pl.when(beside(m, 1))
            def _():
                copy_z(m, c).wait_send()

    loop(0, owners, lambda d: unless_me(lead + d, lambda: collect(d, me).wait_send()))
    loop(0, owners, lambda d: unless_me(lead + d, lambda: hand_out(d, 1).wait_recv()))

    @pl.when(owning)
    def _():
        loop(1, everyone, lambda off: hand_out(rank_of, off).wait_send())

    for d in range(owners):
        out_ref[size + d * part : size + (d + 1) * part, :] = result[d]


def finish_kernel(order_ref, raw_ref, mass_ref, state_ref, in_ref, out_ref):
    ins, size = in_ref.shape
    outs = out_ref.shape[0]
    kept = order_ref[0]
    row = lax.broadcasted_iota(jnp.int32, (size, size), 0)
    col = lax.broadcasted_iota(jnp.int32, (size, size), 1)
    square = jnp.where(jnp.logical_and(row < kept, col < kept), 1.0, 0.0)
    mass_ref[...] = square * raw_ref[:size, :]
    state_ref[...] = square * raw_ref[size : 2 * size, :]
    lanes = jnp.where(col[: ins + outs, :] < kept, 1.0, 0.0)
    lanes = lanes * raw_ref[2 * size : 2 * size + ins + outs, :]
    in_ref[...] = lanes[:ins, :]
    out_ref[...] = lanes[ins:, :]


def on_device(factor_obs, factor_ctrl, diffusivity, input_map, output_map, start_block, order):
    nslab, nsub = lax.axis_size("slab"), lax.axis_size("sub")
    planes, lines, points, wide = factor_ctrl.shape
    cells, plane_cells = planes * lines * points, lines * points
    rank, size = start_block.shape
    ins, outs = input_map.shape[0], output_map.shape[0]
    everyone = nslab * nsub
    step = plane_cells // (2 if lines % 2 == 0 else 1)
    nfar, turns = far_count(nslab), len(sub_bits(nsub)) + 1
    tiles, piece = wide // LANES, wide // 2**turns // nfar
    blocked = pltpu.VMEM((tiles, *(2,) * turns, nfar, piece, LANES), jnp.float32)
    part = -(-(size + ins + outs) // max(everyone // 2, 1))
    owners = -(-(size + ins + outs) // part)
    chunks = face_chunks(plane_cells)
    side = planes * points
    f32, bf16 = jnp.float32, jnp.bfloat16
    vmem, anywhere = pl.BlockSpec(memory_space=pltpu.VMEM), pl.BlockSpec(memory_space=pl.ANY)
    near, far = pltpu.SemaphoreType.DMA((tiles, turns)), pltpu.SemaphoreType.DMA((tiles, nfar))
    every = pltpu.SemaphoreType.DMA((everyone,))
    zs, ys = pltpu.SemaphoreType.DMA((2, chunks)), pltpu.SemaphoreType.DMA((2,))
    early = EARLY_LINES * points
    faces_z = pltpu.VMEM((2, chunks, (plane_cells - early) // chunks, size), f32)
    faces_y = pltpu.VMEM((2, side, size), f32)
    pieces = pltpu.VMEM((everyone, part, LANES), f32)
    owned = pltpu.VMEM((owners, part, LANES), f32)
    raw = pl.pallas_call(
        functools.partial(whole_kernel, nslab, nsub, points, 2),
        out_shape=jax.ShapeDtypeStruct((size + owners * part, size), f32),
        in_specs=[anywhere] * 6,
        out_specs=vmem,
        scratch_shapes=[
            pltpu.VMEM((cells, wide), f32),
            pltpu.VMEM((cells, wide), f32),
            pltpu.VMEM((planes, plane_cells), f32),
            pltpu.VMEM(input_map.shape, f32),
            pltpu.VMEM(output_map.shape, f32),
            pltpu.VMEM((rank, size), f32),
            pltpu.VMEM((cells, LANES), f32),
            pltpu.VMEM((step, wide), bf16),
            pltpu.VMEM((step, wide), bf16),
            pltpu.VMEM((wide, wide), f32),
            pltpu.VMEM((wide, wide), f32),
            pltpu.VMEM((ins + outs, wide), f32),
            blocked, blocked,
            pltpu.VMEM((tiles, nfar, piece, LANES), f32),
        ]
        + [
            pltpu.VMEM((tiles, *(2,) * (turns - 1 - s), nfar, piece, LANES), f32)
            for s in range(turns)
        ]
        + [
            pltpu.VMEM((2, rank, rank), bf16),
            pltpu.VMEM((2, rank, rank), bf16),
            pltpu.VMEM((rank, size), f32),
            pltpu.VMEM((rank, size), f32),
            pltpu.VMEM((size, 2 * size), f32),
            pltpu.VMEM((size, size), f32),
            pltpu.VMEM((size, size), f32),
            faces_z, faces_y, faces_z, faces_y, owned, pieces, owned,
            pltpu.VMEM((2, early, wide), f32),
            pltpu.SemaphoreType.DMA((2, cells // step)),
            pltpu.SemaphoreType.DMA((4,)),
            ys, ys,
            near, near, far, far, far, far, near, near,
            zs, zs, ys, ys, every, every, every, every,
        ],
        compiler_params=pltpu.CompilerParams(
            collective_id=0, has_side_effects=True, vmem_limit_bytes=VMEM_BYTES
        ),
    )(
        factor_obs.reshape(cells, wide),
        factor_ctrl.reshape(cells, wide),
        diffusivity,
        input_map,
        output_map,
        start_block,
    )
    mass, state, seen, felt = pl.pallas_call(
        finish_kernel,
        out_shape=[
            jax.ShapeDtypeStruct((size, size), f32),
            jax.ShapeDtypeStruct((size, size), f32),
            jax.ShapeDtypeStruct((ins, size), f32),
            jax.ShapeDtypeStruct((outs, size), f32),
        ],
        in_specs=[pl.BlockSpec(memory_space=pltpu.SMEM), vmem],
        out_specs=[vmem] * 4,
    )(order, raw)
    return mass, state, seen.T, felt


def solution(mesh):
    placed = (
        P("slab", "sub", None, None),
        P("slab", "sub", None, None),
        P("slab", "sub"),
        P(None, "slab", "sub"),
        P(None, "slab", "sub"),
        P(),
        P(),
    )
    return jax.shard_map(
        on_device, mesh=mesh, in_specs=placed, out_specs=(P(), P(), P(), P()), check_vma=False
    )
```

```python
import functools
import jax
import jax.numpy as jnp
from jax import lax
from jax.experimental import pallas as pl
from jax.experimental.pallas import tpu as pltpu
from jax.sharding import PartitionSpec as P

LANES = 128
SUBS = 8
PANEL = 16
VMEM_BYTES = 60 * 1024 * 1024
EARLY_LINES = 1
SHARES = (1, 1, 1, 1, 1, 1)
HIGHEST = lax.Precision.HIGHEST


def exact(first, second, dims=((1,), (0,))):
    return lax.dot_general(
        first, second, (dims, ((), ())), precision=HIGHEST, preferred_element_type=jnp.float32
    )


def narrow(first, second, dims=((1,), (0,))):
    return lax.dot_general(first, second, (dims, ((), ())), preferred_element_type=jnp.float32)


def three_parts(value):
    high = value.astype(jnp.bfloat16).astype(jnp.float32)
    mid = (value - high).astype(jnp.bfloat16).astype(jnp.float32)
    return high, mid, value - high - mid


def two_parts(value):
    high = value.astype(jnp.bfloat16)
    return high, (value - high.astype(jnp.float32)).astype(jnp.bfloat16)


def three_dots(first, second, dims=((1,), (0,))):
    (a, b), (c, d) = two_parts(first), two_parts(second)
    return narrow(a, c, dims) + (narrow(a, d, dims) + narrow(b, c, dims))


def sub_bits(count):
    return [1 << b for b in range(count.bit_length() - 1)]


def far_count(nslab):
    return max(nslab // 2, 1)


def face_chunks(cells):
    return 2 if cells % 16 == 0 else 1


def thin_dot(rows, high, low):
    above, below = two_parts(rows)
    stack = jnp.concatenate([above.astype(jnp.float32), below.astype(jnp.float32)], axis=0)
    both = narrow(stack.astype(jnp.bfloat16), high)
    count = rows.shape[0]
    return both[:count] + (both[count:] + narrow(above, low))


def across(block, sub):
    return jnp.broadcast_to(block[sub : sub + 1, :], block.shape)

def column(rows, lane):
    return jnp.broadcast_to(rows[:, lane : lane + 1], (SUBS, LANES))

def inverse_factor(work, size):
    wide = 2 * size // LANES
    place = lax.broadcasted_iota(jnp.int32, (SUBS, 2 * size), 0)
    spread = lambda x: jnp.concatenate([x] * wide, axis=1)
    carried = [work[h * SUBS : (h + 1) * SUBS, :] for h in range(2)]
    for base in range(0, size, PANEL):
        low, high = carried
        cols_low = [column(low, base + j) for j in range(SUBS)]
        cols_high = [column(high, base + j) for j in range(PANEL)]
        panel_low, panel_high = low, high
        scales, rows, leads = [], [], []
        for j in range(PANEL):
            if j < SUBS:
                scale = lax.rsqrt(across(cols_low[j], j))
                lead_low = cols_low[j] * scale
                row = across(low, j) * spread(scale)
                panel_low = jnp.where(place == j, row, panel_low)
            else:
                scale = lax.rsqrt(across(cols_high[j], j - SUBS))
                row = across(high, j - SUBS) * spread(scale)
                panel_high = jnp.where(place == j - SUBS, row, panel_high)
            lead_high = cols_high[j] * scale
            lead = {}
            for m in range(j + 1, PANEL):
                if m < SUBS:
                    lead[m] = across(lead_low, m)
                    cols_low[m] = cols_low[m] - lead_low * lead[m]
                else:
                    lead[m] = across(lead_high, m - SUBS)
                cols_high[m] = cols_high[m] - lead_high * lead[m]
            if j < SUBS - 1:
                low = low - spread(lead_low) * row
            if j < PANEL - 1:
                high = high - spread(lead_high) * row
            scales.append(scale)
            rows.append(row)
            leads.append(lead)
        panel = jnp.concatenate([panel_low, panel_high], axis=0)
        work[base : base + PANEL, :] = panel
        if base + PANEL < size:
            start = base + PANEL
            carried = []
            for h in range(2):
                rest = work[start + h * SUBS : start + (h + 1) * SUBS, :]
                cols = [column(rest, base + j) for j in range(PANEL)]
                for j in range(PANEL):
                    lead_rest = cols[j] * scales[j]
                    for m in range(j + 1, PANEL):
                        cols[m] = cols[m] - lead_rest * leads[j][m]
                    rest = rest - spread(lead_rest) * rows[j]
                carried.append(rest)
        if base + 2 * PANEL < size:
            start = base + 2 * PANEL
            high, mid, low = three_parts(panel)
            first = jnp.concatenate([high, high, mid, high, low, mid], axis=0)[:, :size]
            second = jnp.concatenate([high, mid, high, low, high, mid], axis=0)
            update = narrow(first.astype(jnp.bfloat16), second.astype(jnp.bfloat16), ((0,), (0,)))
            work[start:, :] = work[start:, :] - update[start:, :]


def pair(value):
    return jnp.concatenate(two_parts(value), axis=1)


def fold(wide, size):
    return wide[:, :size] + wide[:, size:]


def apply_parts(high, low, block):
    size = block.shape[1]
    parts = pair(block)
    return fold(narrow(high, parts) + narrow(low, parts), size)


def gram_parts(parts):
    size = parts.shape[1] // 2
    full = narrow(parts, parts, ((0,), (0,)))
    return (full[:size, :size] + full[size:, size:]) + (full[:size, size:] + full[size:, :size])


def right_apply(parts, factor):
    turned = pair(factor.T)
    return fold(narrow(parts, jnp.concatenate([turned, turned], axis=0)), factor.shape[0])


def peers(slab, sub, nslab, nsub):
    everyone, me = nslab * nsub, slab * nsub + sub

    def peer(off):
        other = lax.rem(me + off, everyone)
        return other, {"slab": other // nsub, "sub": lax.rem(other, nsub)}

    return everyone, me, peer


def whole_kernel(nslab, nsub, points, sweeps, *refs):
    obs_hbm, ctrl_hbm, conduct_hbm, drive_hbm, sense_hbm, start_hbm, out_ref = refs[:7]
    obs, ctrl, conduct, drive, sense, start, spread_k, applied_high, applied_low = refs[7:16]
    turns = [("sub", bit) for bit in sub_bits(nsub)] + [("slab", 1)]
    refs = list(refs[16:])

    def take(count):
        return [refs.pop(0) for _ in range(count)]

    acc, inner, maps, work, whole, got_far = take(6)
    got = take(len(turns))
    both_high, both_low, left, right, product, square, turned, face = take(8)
    send_z, send_y, got_z, got_y, pack, slots, result = take(7)
    raw_z, image0, load, load_small, raw_send, raw_recv, image_send, image_recv = take(8)
    rs_send, rs_recv, far_send, far_recv, back_send, back_recv, ag_send, ag_recv = take(8)
    z_send, z_recv, y_send, y_recv, sum_send, sum_recv, give_send, give_recv = take(8)
    slab, sub = lax.axis_index("slab"), lax.axis_index("sub")
    everyone, me, peer = peers(slab, sub, nslab, nsub)
    cells, wide = ctrl.shape
    planes, plane_cells = conduct.shape
    step = applied_high.shape[0]
    count = cells // step
    nfar = far_count(nslab)

    def fetch(which, k):
        rows = pl.ds(k * step, step)
        source, target = ((obs_hbm, obs), (ctrl_hbm, ctrl))[which]
        return pltpu.make_async_copy(source.at[rows], target.at[rows], load.at[which, k])

    places = (("slab", slab, nslab, 1), ("slab", slab, nslab, -1))
    places = places + (("sub", sub, nsub, 1), ("sub", sub, nsub, -1))

    def beside(m, way):
        _, index, count, step = places[m]
        return index < count - 1 if step * way > 0 else index > 0

    def copy_raw(m):
        axis, index, _, way = places[m]
        first = (1 - m) * (planes - 1) * plane_cells
        return pltpu.make_async_remote_copy(
            src_ref=ctrl_hbm.at[pl.ds(first, raw_z.shape[1])],
            dst_ref=raw_z.at[m],
            send_sem=raw_send.at[m],
            recv_sem=raw_recv.at[m],
            device_id={axis: index + way},
        )

    small = [
        pltpu.make_async_copy(here, there, load_small.at[i])
        for i, (here, there) in enumerate(
            ((conduct_hbm, conduct), (drive_hbm, drive), (sense_hbm, sense), (start_hbm, start))
        )
    ]
    small[0].start()
    ahead = min(2, count)
    for k in range(ahead):
        fetch(0, k).start()
        fetch(1, k).start()
    for copy in small[1:]:
        copy.start()

    def partner(axis, bit):
        index = slab if axis == "slab" else sub
        has = lax.rem(index // bit, 2)
        return has, {axis: index + bit - 2 * bit * has}

    def far(off):
        other = lax.rem(slab // 2 + off, nfar)
        return other, {"slab": other * 2 + lax.rem(slab, 2)}

    barrier = pltpu.get_barrier_semaphore()

    def greet(off, carry):
        pl.semaphore_signal(barrier, inc=1, device_id=peer(off)[1])
        return carry

    lax.fori_loop(1, everyone, greet, 0)
    small[0].wait()
    for p in range(planes):
        for c in range(plane_cells // LANES):
            lanes = conduct[p : p + 1, c * LANES : (c + 1) * LANES] * (1.0 / 6.0)
            first = p * plane_cells + c * LANES
            spread_k[first : first + LANES, :] = jnp.broadcast_to(lanes, (LANES, LANES)).T
    acc[...] = jnp.zeros_like(acc)

    def add_block(k, carry):
        fetch(0, k).wait()
        fetch(1, k).wait()

        @pl.when(k + ahead < count)
        def _():
            fetch(0, k + ahead).start()
            fetch(1, k + ahead).start()

        rows = pl.ds(pl.multiple_of(k * step, step), step)
        acc[...] += three_dots(ctrl[rows, :], obs[rows, :], ((0,), (0,)))
        return carry

    lax.fori_loop(0, 1, add_block, 0)
    pl.semaphore_wait(barrier, everyone - 1)
    for m in range(2):

        @pl.when(beside(m, 1))
        def _():
            copy_raw(m).start()

        @pl.when(jnp.logical_not(beside(m, -1)))
        def _():
            raw_z[m] = jnp.zeros(raw_z.shape[1:], jnp.float32)

    lax.fori_loop(1, count, add_block, 0)
    blocked = work.shape[1:]
    for c in range(acc.shape[1] // LANES):
        work[c] = acc[:, c * LANES : (c + 1) * LANES].reshape(blocked)
    for copy in small[1:]:
        copy.wait()

    place = lax.broadcasted_iota(jnp.int32, (points, wide), 0)

    def inner_block(k):
        first = k * step
        plane = first // plane_cells

        ends = ((0, 0), (1, planes - 1))
        sides = [m for m, at in ends if at == plane and first % plane_cells == 0]
        for m in sides:

            @pl.when(beside(m, -1))
            def _():
                copy_raw(m).wait_recv()

        def line(i, carry, sides=()):
            row = pl.multiple_of(first + i * points, points)
            within = lax.rem(row, plane_cells)
            here = ctrl[pl.ds(row, points), :]
            total = jnp.where(place > 0, pltpu.roll(here, 1, 0), 0.0)
            total = total + jnp.where(place < points - 1, pltpu.roll(here, points - 1, 0), 0.0)
            before = pl.multiple_of(jnp.maximum(row - points, 0), points)
            after = pl.multiple_of(jnp.minimum(row + points, cells - points), points)
            total = total + jnp.where(within > 0, 1.0, 0.0) * ctrl[pl.ds(before, points), :]
            inside = jnp.where(within < plane_cells - points, 1.0, 0.0)
            total = total + inside * ctrl[pl.ds(after, points), :]
            if plane > 0:
                total = total + ctrl[pl.ds(row - plane_cells, points), :]
            if plane < planes - 1:
                total = total + ctrl[pl.ds(row + plane_cells, points), :]
            for m in sides:
                total = total + raw_z[m, pl.ds(pl.multiple_of(i * points, points), points), :]
            scale = jnp.concatenate([spread_k[pl.ds(row, points), :]] * (wide // LANES), axis=1)
            high, low = two_parts(scale * (total - 6.0 * here))
            applied_high[pl.ds(pl.multiple_of(i * points, points), points), :] = high
            applied_low[pl.ds(pl.multiple_of(i * points, points), points), :] = low
            return carry

        extra = raw_z.shape[1] // points if sides else 0
        if sides:
            lax.fori_loop(0, extra, functools.partial(line, sides=sides), 0)
        lax.fori_loop(extra, step // points, line, 0)
        rows = slice(first, first + step)
        high, low = two_parts(obs[rows, :])
        dims = ((0,), (0,))
        value = narrow(high, applied_high[...], dims) + (
            narrow(high, applied_low[...], dims) + narrow(low, applied_high[...], dims)
        )
        lanes = slice(first % plane_cells, first % plane_cells + step)
        seen = thin_dot(drive[:, plane, lanes], high, low)
        felt = thin_dot(sense[:, plane, lanes], *two_parts(ctrl[rows, :]))
        both = jnp.concatenate([seen, felt], axis=0)
        if k == sequence[0]:
            inner[...] = value
            maps[...] = both
        else:
            inner[...] += value
            maps[...] += both

    per_plane = plane_cells // step
    late = [0, (planes - 1) * per_plane]
    sequence = [k for k in range(count) if k not in late] + late
    blocks = iter(sequence)

    def work_meanwhile(amount):
        for _ in range(amount):
            k = next(blocks, None)
            if k is not None:
                inner_block(k)

    tiles = work.shape[0]
    here = [partner(axis, bit)[0] for axis, bit in turns]
    orders = [list(range(len(turns))) for _ in range(tiles)]
    for c in range(1, tiles, 2):
        orders[c] = orders[c][:1] + orders[c][1:][::-1]

    def region(c, done, flip=None):
        index = [slice(None)] * len(turns)
        for t in done:
            index[t] = here[t]
        if flip is not None:
            index[flip] = 1 - here[flip]
        return (c, *index)

    def halve(c, s):
        t = orders[c][s]
        return pltpu.make_async_remote_copy(
            src_ref=work.at[region(c, orders[c][:s], t)],
            dst_ref=got[s].at[c],
            send_sem=rs_send.at[c, s],
            recv_sem=rs_recv.at[c, s],
            device_id=partner(*turns[t])[1],
        )

    def scatter(c, off):
        other, target = far(off)
        return pltpu.make_async_remote_copy(
            src_ref=work.at[(c, *here, other)],
            dst_ref=got_far.at[c, off],
            send_sem=far_send.at[c, off],
            recv_sem=far_recv.at[c, off],
            device_id=target,
        )

    def gather_far(c, off):
        return pltpu.make_async_remote_copy(
            src_ref=whole.at[(c, *here, slab // 2)],
            dst_ref=whole.at[(c, *here, slab // 2)],
            send_sem=back_send.at[c, off],
            recv_sem=back_recv.at[c, off],
            device_id=far(off)[1],
        )

    def double(c, s):
        mine = region(c, orders[c][: s + 1])
        return pltpu.make_async_remote_copy(
            src_ref=whole.at[mine],
            dst_ref=whole.at[mine],
            send_sem=ag_send.at[c, s],
            recv_sem=ag_recv.at[c, s],
            device_id=partner(*turns[orders[c][s]])[1],
        )

    last = len(turns) - 1
    for s in range(len(turns)):
        for c in range(tiles):
            if s:
                halve(c, s - 1).wait()
                work[region(c, orders[c][:s])] += got[s - 1][c]
            halve(c, s).start()
        work_meanwhile(SHARES[s])
    for c in range(tiles):
        halve(c, last).wait()
        work[(c, *here)] += got[last][c]
        for off in range(1, nfar):
            scatter(c, off).start()
    work_meanwhile(SHARES[-3])
    for c in range(tiles):
        total = work[(c, *here, slab // 2)]
        for off in range(1, nfar):
            scatter(c, off).wait()
            total = total + got_far[c, off]
        whole[(c, *here, slab // 2)] = total
        for off in range(1, nfar):
            gather_far(c, off).start()

    def broadcast(off):
        return pltpu.make_async_remote_copy(
            src_ref=image0.at[(*here, slab // 2)],
            dst_ref=image0.at[(*here, slab // 2)],
            send_sem=image_send.at[off],
            recv_sem=image_recv.at[off],
            device_id=peer(off)[1],
        )

    def loop(first, stop, act):
        def body(i, carry):
            act(i)
            return carry

        lax.fori_loop(first, stop, body, 0)

    slices = [whole[(c, *here, slab // 2)] for c in range(tiles)]
    image0[(*here, slab // 2)] = three_dots(jnp.concatenate(slices, axis=1), start[...])
    loop(1, everyone // 2, lambda off: broadcast(2 * off).start())

    def advance(s):
        for c in range(tiles):
            if s == last:
                for off in range(1, nfar):
                    gather_far(c, off).wait()
            else:
                double(c, s + 1).wait()
            double(c, s).start()

    work_meanwhile(SHARES[-2])
    advance(last)
    work_meanwhile(SHARES[-1])
    loop(1, everyone // 2, lambda off: broadcast(2 * off).wait())
    swap = pltpu.make_async_remote_copy(
        src_ref=image0.at[here[0]],
        dst_ref=image0.at[here[0]],
        send_sem=image_send.at[0],
        recv_sem=image_recv.at[0],
        device_id=partner(*turns[0])[1],
    )
    swap.start()
    for s in reversed(range(1, last)):
        advance(s)
    swap.wait()

    rank, size = start.shape
    chunks = face_chunks(plane_cells)
    early = raw_z.shape[1]
    chunk = (plane_cells - early) // chunks

    def edge_lines(ref, side):
        firsts = [p * plane_cells + side * (plane_cells - points) for p in range(planes)]
        return jnp.concatenate([ref[first : first + points, :] for first in firsts], axis=0)

    row = lax.broadcasted_iota(jnp.int32, (size, size), 0)
    col = lax.broadcasted_iota(jnp.int32, (size, size), 1)
    eye = (row == col).astype(jnp.float32)

    def copy_z(m, c):
        axis, index, _, step = places[m]
        return pltpu.make_async_remote_copy(
            src_ref=send_z.at[m, c],
            dst_ref=got_z.at[m, c],
            send_sem=z_send.at[m, c],
            recv_sem=z_recv.at[m, c],
            device_id={axis: index + step},
        )

    def copy_y(m):
        axis, index, _, step = places[2 + m]
        return pltpu.make_async_remote_copy(
            src_ref=send_y.at[m],
            dst_ref=got_y.at[m],
            send_sem=y_send.at[m],
            recv_sem=y_recv.at[m],
            device_id={axis: index + step},
        )

    def project(cells, parts):
        high, low = two_parts(cells)
        return fold(narrow(high, parts) + narrow(low, parts), size)

    def send_faces():
        parts = pair(apply_parts(both_high[1], both_low[1], left[...]))
        image = narrow(both_high[0], parts) + narrow(both_low[0], parts)
        parts = pair(fold(image, size))
        for c in range(chunks):
            for m in range(2):
                first = (1 - m) * (planes - 1) * plane_cells + early + c * chunk
                send_z[m, c] = project(ctrl[first : first + chunk, :], parts)

                @pl.when(beside(m, 1))
                def _():
                    copy_z(m, c).start()

        for m in range(2):
            send_y[m] = project(edge_lines(ctrl, 1 - m), parts)

            @pl.when(beside(2 + m, 1))
            def _():
                copy_y(m).start()

    def sweep(k, carry):
        turn = lax.rem(k, 2)

        @pl.when(k == 0)
        def _():
            product[...] = image0[...].reshape(rank, size)

        @pl.when(k > 0)
        def _():
            product[...] = apply_parts(both_high[turn], both_low[turn], left[...])

        parts = pair(product[...])
        square[:, :size] = gram_parts(parts)
        square[:, size:] = eye
        inverse_factor(square, size)
        right[...] = left[...]
        left[...] = right_apply(parts, square[:, size:])

        @pl.when(k == 0)
        def _():
            advance(0)
            for c in range(tiles):
                double(c, 0).wait()
                cols = slice(c * LANES, (c + 1) * LANES)
                tile = whole[c].reshape(rank, LANES)
                high, low = two_parts(tile)
                both_high[0, :, cols] = high
                both_low[0, :, cols] = low
                high, low = two_parts(tile.T)
                both_high[1, cols, :] = high
                both_low[1, cols, :] = low
            send_faces()
            turned[...] = eye

        @pl.when(jnp.logical_and(k > 0, k < 2 * sweeps - 1))
        def _():
            turned[...] = exact(turned[...], square[:, size:], ((1,), (1,)))

        return carry

    left[...] = start[...]
    lax.fori_loop(0, 2 * sweeps, sweep, 0)

    work_meanwhile(count)
    left_parts, right_parts = pair(left[...]), pair(right[...])
    image = fold(narrow(both_high[1], right_parts) + narrow(both_low[1], right_parts), size)
    out_ref[:size, :] = exact(left[...], image, ((0,), (0,)))
    state = exact(left[...], project(inner[...], right_parts), ((0,), (0,)))
    ins, both_maps = drive.shape[0], maps.shape[0]
    seen = project(maps[...], left_parts)
    felt = project(maps[...], right_parts)
    side = lax.broadcasted_iota(jnp.int32, seen.shape, 0)
    out_ref[2 * size :, :] = jnp.zeros((out_ref.shape[0] - 2 * size, size), jnp.float32)
    out_ref[2 * size : 2 * size + both_maps, :] = jnp.where(side < ins, seen, felt)

    face[...] = jnp.zeros_like(face)
    for m in range(2):
        mine = project(edge_lines(obs, m), left_parts) * edge_lines(spread_k, m)

        @pl.when(beside(2 + m, -1))
        def _():
            copy_y(m).wait_recv()
            face[...] += three_dots(mine, got_y[m], ((0,), (0,)))

    for c in range(chunks):
        for m in range(2):
            first = m * (planes - 1) * plane_cells + early + c * chunk
            rows = slice(first, first + chunk)
            mine = project(obs[rows, :], left_parts) * spread_k[rows, :]

            @pl.when(beside(m, -1))
            def _():
                copy_z(m, c).wait_recv()
                face[...] += three_dots(mine, got_z[m, c], ((0,), (0,)))

    out_ref[size : 2 * size, :] = state + exact(face[...], turned[...])
    owners, part = pack.shape[:2]
    lead = (nslab // 4) * nsub
    rank_of = me - lead
    owning = jnp.logical_and(rank_of >= 0, rank_of < owners)
    for d in range(owners):
        pack[d] = out_ref[size + d * part : size + (d + 1) * part, :]

    def device(linear):
        return {"slab": linear // nsub, "sub": lax.rem(linear, nsub)}

    def collect(owner, source):
        return pltpu.make_async_remote_copy(
            src_ref=pack.at[owner],
            dst_ref=slots.at[source],
            send_sem=sum_send.at[owner],
            recv_sem=sum_recv.at[source],
            device_id=device(lead + owner),
        )

    def hand_out(owner, off):
        return pltpu.make_async_remote_copy(
            src_ref=result.at[owner],
            dst_ref=result.at[owner],
            send_sem=give_send.at[off],
            recv_sem=give_recv.at[owner],
            device_id=peer(off)[1],
        )

    def unless_me(linear, act):
        @pl.when(linear != me)
        def _():
            act()

    loop(0, owners, lambda d: unless_me(lead + d, lambda: collect(d, me).start()))

    @pl.when(owning)
    def _():
        slots[me] = pack[rank_of]
        loop(0, everyone, lambda i: unless_me(i, lambda: collect(0, i).wait_recv()))
        result[rank_of] = jnp.sum(slots[...], axis=0)
        loop(1, everyone, lambda off: hand_out(rank_of, off).start())

    for m in range(2):

        @pl.when(beside(m, 1))
        def _():
            copy_raw(m).wait_send()

        @pl.when(beside(2 + m, 1))
        def _():
            copy_y(m).wait_send()

        for c in range(chunks):

            @pl.when(beside(m, 1))
            def _():
                copy_z(m, c).wait_send()

    loop(0, owners, lambda d: unless_me(lead + d, lambda: collect(d, me).wait_send()))
    loop(0, owners, lambda d: unless_me(lead + d, lambda: hand_out(d, 1).wait_recv()))

    @pl.when(owning)
    def _():
        loop(1, everyone, lambda off: hand_out(rank_of, off).wait_send())

    for d in range(owners):
        out_ref[size + d * part : size + (d + 1) * part, :] = result[d]


def finish_kernel(order_ref, raw_ref, mass_ref, state_ref, in_ref, out_ref):
    ins, size = in_ref.shape
    outs = out_ref.shape[0]
    kept = order_ref[0]
    row = lax.broadcasted_iota(jnp.int32, (size, size), 0)
    col = lax.broadcasted_iota(jnp.int32, (size, size), 1)
    square = jnp.where(jnp.logical_and(row < kept, col < kept), 1.0, 0.0)
    mass_ref[...] = square * raw_ref[:size, :]
    state_ref[...] = square * raw_ref[size : 2 * size, :]
    lanes = jnp.where(col[: ins + outs, :] < kept, 1.0, 0.0)
    lanes = lanes * raw_ref[2 * size : 2 * size + ins + outs, :]
    in_ref[...] = lanes[:ins, :]
    out_ref[...] = lanes[ins:, :]


def on_device(factor_obs, factor_ctrl, diffusivity, input_map, output_map, start_block, order):
    nslab, nsub = lax.axis_size("slab"), lax.axis_size("sub")
    planes, lines, points, wide = factor_ctrl.shape
    cells, plane_cells = planes * lines * points, lines * points
    rank, size = start_block.shape
    ins, outs = input_map.shape[0], output_map.shape[0]
    everyone = nslab * nsub
    step = plane_cells // (2 if lines % 2 == 0 else 1)
    nfar, turns = far_count(nslab), len(sub_bits(nsub)) + 1
    tiles, piece = wide // LANES, wide // 2**turns // nfar
    blocked = pltpu.VMEM((tiles, *(2,) * turns, nfar, piece, LANES), jnp.float32)
    part = -(-(size + ins + outs) // max(everyone // 2, 1))
    owners = -(-(size + ins + outs) // part)
    chunks = face_chunks(plane_cells)
    side = planes * points
    f32, bf16 = jnp.float32, jnp.bfloat16
    vmem, anywhere = pl.BlockSpec(memory_space=pltpu.VMEM), pl.BlockSpec(memory_space=pl.ANY)
    near, far = pltpu.SemaphoreType.DMA((tiles, turns)), pltpu.SemaphoreType.DMA((tiles, nfar))
    every = pltpu.SemaphoreType.DMA((everyone,))
    zs, ys = pltpu.SemaphoreType.DMA((2, chunks)), pltpu.SemaphoreType.DMA((2,))
    early = EARLY_LINES * points
    faces_z = pltpu.VMEM((2, chunks, (plane_cells - early) // chunks, size), f32)
    faces_y = pltpu.VMEM((2, side, size), f32)
    pieces = pltpu.VMEM((everyone, part, LANES), f32)
    owned = pltpu.VMEM((owners, part, LANES), f32)
    raw = pl.pallas_call(
        functools.partial(whole_kernel, nslab, nsub, points, 2),
        out_shape=jax.ShapeDtypeStruct((size + owners * part, size), f32),
        in_specs=[anywhere] * 6,
        out_specs=vmem,
        scratch_shapes=[
            pltpu.VMEM((cells, wide), f32),
            pltpu.VMEM((cells, wide), f32),
            pltpu.VMEM((planes, plane_cells), f32),
            pltpu.VMEM(input_map.shape, f32),
            pltpu.VMEM(output_map.shape, f32),
            pltpu.VMEM((rank, size), f32),
            pltpu.VMEM((cells, LANES), f32),
            pltpu.VMEM((step, wide), bf16),
            pltpu.VMEM((step, wide), bf16),
            pltpu.VMEM((wide, wide), f32),
            pltpu.VMEM((wide, wide), f32),
            pltpu.VMEM((ins + outs, wide), f32),
            blocked, blocked,
            pltpu.VMEM((tiles, nfar, piece, LANES), f32),
        ]
        + [
            pltpu.VMEM((tiles, *(2,) * (turns - 1 - s), nfar, piece, LANES), f32)
            for s in range(turns)
        ]
        + [
            pltpu.VMEM((2, rank, rank), bf16),
            pltpu.VMEM((2, rank, rank), bf16),
            pltpu.VMEM((rank, size), f32),
            pltpu.VMEM((rank, size), f32),
            pltpu.VMEM((rank, size), f32),
            pltpu.VMEM((size, 2 * size), f32),
            pltpu.VMEM((size, size), f32),
            pltpu.VMEM((size, size), f32),
            faces_z, faces_y, faces_z, faces_y, owned, pieces, owned,
            pltpu.VMEM((2, early, wide), f32),
            pltpu.VMEM((*(2,) * turns, nfar, piece, size), f32),
            pltpu.SemaphoreType.DMA((2, cells // step)),
            pltpu.SemaphoreType.DMA((4,)),
            ys, ys, every, every,
            near, near, far, far, far, far, near, near,
            zs, zs, ys, ys, every, every, every, every,
        ],
        compiler_params=pltpu.CompilerParams(
            collective_id=0, has_side_effects=True, vmem_limit_bytes=VMEM_BYTES
        ),
    )(
        factor_obs.reshape(cells, wide),
        factor_ctrl.reshape(cells, wide),
        diffusivity,
        input_map,
        output_map,
        start_block,
    )
    mass, state, seen, felt = pl.pallas_call(
        finish_kernel,
        out_shape=[
            jax.ShapeDtypeStruct((size, size), f32),
            jax.ShapeDtypeStruct((size, size), f32),
            jax.ShapeDtypeStruct((ins, size), f32),
            jax.ShapeDtypeStruct((outs, size), f32),
        ],
        in_specs=[pl.BlockSpec(memory_space=pltpu.SMEM), vmem],
        out_specs=[vmem] * 4,
    )(order, raw)
    return mass, state, seen.T, felt


def solution(mesh):
    placed = (
        P("slab", "sub", None, None),
        P("slab", "sub", None, None),
        P("slab", "sub"),
        P(None, "slab", "sub"),
        P(None, "slab", "sub"),
        P(),
        P(),
    )
    return jax.shard_map(
        on_device, mesh=mesh, in_specs=placed, out_specs=(P(), P(), P(), P()), check_vma=False
    )
```
